128 devices in a mesh: ep: 8 (over x, core), tp: 16 (over z, y).
Axes of the slice: x: 4, y: 4, z: 4, core: 2. Of those that a mesh axis runs over, the one named last changes fastest.
Arguments:
- layer_input: bfloat16 [2048, 4096], P('ep', 'tp'), may hold values from -6 to 6
- out_grad: bfloat16 [2048, 4096], P('ep', 'tp'), may hold values from -6 to 6
- route: int32 [2048, 2], P('ep'), may hold values from 0 to 7, all different within a row; in each aligned block of 256 rows (0 to 255, 256 to 511, ...) at most 96 rows name the same one
- gate_share: float32 [2048, 2], P('ep'), may hold values from 0.2 to 1
- gate_weight: bfloat16 [8, 4096, 14336], P('ep', None, 'tp'), may hold values from -0.125 to 0.125
- up_weight: bfloat16 [8, 4096, 14336], P('ep', None, 'tp'), may hold values from -0.125 to 0.125
- down_weight: bfloat16 [8, 14336, 4096], P('ep', 'tp'), may hold values from -0.046875 to 0.046875
Outputs:
- input_grad: bfloat16 [2048, 4096], P('ep', 'tp')
The draws below stay inside these ranges and needn't reach their ends.
Inputs may be any that keep to these rules, and one draw needn't show every extreme that they name: `route`: each row names 2 different experts. In each aligned block of 256 rows (the rows of one index of ep) no expert is named by more than 96 rows, a bound that some block reaches.
All inputs are finite; a program needn't handle non-finite values.
Results may differ from the reference program's by a relative error of at most 0.0057.
Values may be sent and summed in bfloat16 or wider, within the bound.
No kernel may reach another device: no remote copies, remote signals or barrier semaphores. Data moves between devices by JAX's collectives and lax.ppermute only.
A program may use at most 320 MiB of HBM per device.

```python
import math
import jax
import jax.numpy as jnp
import numpy as np
from jax import lax

D = 4096
FF = 14336
TOP = 2
TOK_EP = 256
EXPERTS = 8
CAP = 96
TOKENS = 2048
N_EP = 8


def with_spikes(result, rng, source, target, blocks, factor):
    def block_of(dim):
        return (jnp.arange(result.shape[dim]) // (result.shape[dim] // blocks)).reshape((-1,) + (1,) * (result.ndim - 1 - dim))

    first = jax.random.permutation(rng, blocks)[block_of(target)]
    second = (block_of(target) + blocks // 2) % blocks
    return jnp.where((block_of(source) == first) | (block_of(source) == second), factor * result, result)


def shard_levels(key, extent, shards, low, high):
    loudness = 1.0
    for dim, blocks in shards:
        heights = jax.random.uniform(jax.random.fold_in(jax.random.fold_in(key, 6), dim), (blocks,), jnp.float32, low / len(shards), high / len(shards))
        loudness = loudness * jnp.repeat(jnp.exp(heights), extent[dim] // blocks).reshape((-1,) + (1,) * (len(extent) - 1 - dim))
    return loudness


def deal_out(rng, own, number, rows, count, top, most, lean):
    sequence = jax.random.permutation(rng, count)
    heavy_load, common = portions_of(count, rows * top, most, lean, True), portions_of(count, rows * top, most, lean, False)
    places = jnp.arange(count)

    def named(tallies, turn):
        used = int((tallies > 0).sum())
        fixed = max(1, used // 4)
        shifted = fixed + (places - fixed + turn * (used - fixed)) % max(1, count - fixed)
        return jnp.zeros((count,), jnp.int32).at[sequence[jnp.where(places < fixed, places, shifted)]].set(jnp.asarray(tallies, jnp.int32))

    tallies = jnp.where(number % 4 == 0, named(heavy_load, number // 4), named(common, number - number // 4 - 1))
    mixed = jax.random.permutation(jax.random.fold_in(own, 3), count)
    donor, receiver = mixed[0:count // 2 * 2:2], mixed[1:count // 2 * 2:2]
    margin = jnp.minimum(tallies[donor] - 1, most - tallies[receiver]) // 2
    margin = jnp.where((donor == sequence[0]) | (receiver == sequence[0]) | (tallies[receiver] == 0), 0, jnp.maximum(margin, 0))
    shifted = jax.random.randint(jax.random.fold_in(own, 4), (count // 2,), 0, 1 << 20) % (margin + 1)
    tallies = tallies.at[donor].add(-shifted).at[receiver].add(shifted)
    items = jnp.searchsorted(jnp.cumsum(tallies), jnp.arange(rows * top), side="right").astype(jnp.int32)
    grid = items.reshape(top, rows).T
    grid = grid[jax.random.permutation(jax.random.fold_in(own, 1), rows)]
    turn = jax.random.randint(jax.random.fold_in(own, 2), (rows, 1), 0, top)
    return jnp.take_along_axis(grid, (jnp.arange(top)[None, :] + turn) % top, axis=1)


def portions_of(count, total, most, lean, full):
    loads = [(1 << 20) // math.isqrt(standing ** lean) + 1 for standing in range(1, count + 1)]
    largest = most if full else min(most, max(-(-total // count), total * loads[0] // sum(loads)))
    least = 1 if total - largest >= count - 1 else 0
    holding, spare = [largest] + [least] * (count - 1), total - largest - least * (count - 1)
    while spare > 0:
        free = [i for i in range(1, count) if holding[i] < largest] or [i for i in range(1, count) if holding[i] < most]
        whole, budget = sum([loads[i] for i in free]), spare
        for i in free:
            addition = min(most - holding[i], max(1, budget * loads[i] // whole), spare)
            holding[i] = holding[i] + addition
            spare = spare - addition
    return np.array(holding)


def centred(stream_key, shape, width, limit, split=(), held_as=jnp.bfloat16):
    values = width * jax.random.normal(stream_key, shape, jnp.float32)
    if split:
        values = values * shard_levels(stream_key, shape, split, -0.22, 0.18)
    return jnp.clip(values, -limit, limit).astype(held_as)


def gaussian_with(stream_key, shape, deviation, limit, pieces, heavy, kind=jnp.bfloat16):
    values = deviation * jax.random.normal(stream_key, shape, jnp.float32)
    if pieces:
        values = values * shard_levels(stream_key, shape, pieces, -0.22, 0.18)
    return jnp.clip(with_spikes(values, jax.random.fold_in(stream_key, 3), *heavy), -limit, limit).astype(kind)


def setup_inputs(seed: int = 0) -> dict:
    seeds = jax.random.split(jax.random.key(seed), 8)
    layer_input = centred(seeds[0], (TOKENS, D), 1.0, 6.0, ((0, 8), (1, 16)))
    out_grad = centred(seeds[1], (TOKENS, D), 1.0, 6.0, ((0, 8), (1, 16)))
    route_keys = jax.random.split(jax.random.fold_in(seeds[2], 1), TOKENS // TOK_EP)
    route_turns = jax.random.permutation(jax.random.fold_in(seeds[2], 3), TOKENS // TOK_EP)
    route = jax.vmap(lambda own, number: deal_out(jax.random.fold_in(seeds[2], 2), own, number, TOK_EP, EXPERTS, TOP, CAP, 2))(route_keys, route_turns).reshape((TOKENS, TOP))
    gate_share = jnp.clip(0.2 + 0.8 * jax.random.uniform(seeds[3], (TOKENS, TOP), jnp.float32) ** shard_levels(seeds[3], (TOKENS, TOP), ((0, 8),), -0.2, 0.2), 0.2, 1.0)
    gate_weight = gaussian_with(seeds[4], (EXPERTS, D, FF), D ** -0.5, 0.125, ((0, 8), (2, 16)), (2, 1, 16, 2.0))
    up_weight = gaussian_with(seeds[5], (EXPERTS, D, FF), D ** -0.5, 0.125, ((0, 8), (2, 16)), (2, 1, 16, 2.0))
    down_weight = centred(seeds[6], (EXPERTS, FF, D), FF ** -0.5, 0.046875, ((0, 8), (1, 16)))
    return {"layer_input": layer_input, "out_grad": out_grad, "route": route, "gate_share": gate_share, "gate_weight": gate_weight, "up_weight": up_weight, "down_weight": down_weight}


def slot_positions(blocks):
    onehot = (blocks[..., None] == jnp.arange(EXPERTS, dtype=jnp.int32)).astype(jnp.int32).sum(axis=2)
    before = jnp.cumsum(onehot, axis=1) - onehot
    return jnp.take_along_axis(before, blocks, axis=2).astype(jnp.int32)


def expert_rows(gate_matrix, up_matrix, down_matrix, inputs, grads):
    gate_act = jnp.dot(inputs, gate_matrix, preferred_element_type=jnp.float32)
    up_act = jnp.dot(inputs, up_matrix, preferred_element_type=jnp.float32)
    hidden_grad = lax.dot_general(grads, down_matrix, (((1,), (1,)), ((), ())), preferred_element_type=jnp.float32)
    sigma = jax.nn.sigmoid(gate_act)
    slope = sigma * (1.0 + gate_act * (1.0 - sigma))
    gate_grad = (hidden_grad * up_act * slope).astype(jnp.bfloat16)
    up_grad = (hidden_grad * gate_act * sigma).astype(jnp.bfloat16)
    total = lax.dot_general(gate_grad, gate_matrix, (((1,), (1,)), ((), ())), preferred_element_type=jnp.float32)
    total = total + lax.dot_general(up_grad, up_matrix, (((1,), (1,)), ((), ())), preferred_element_type=jnp.float32)
    return total.astype(jnp.bfloat16)


def reference(layer_input, out_grad, route, gate_share, gate_weight, up_weight, down_weight):
    blocks = route.reshape(N_EP, TOK_EP, TOP)
    position = slot_positions(blocks)
    flat = blocks * CAP + position
    owner = jnp.broadcast_to(jnp.arange(TOK_EP, dtype=jnp.int32)[None, :, None], flat.shape)
    block_index = jnp.broadcast_to(jnp.arange(N_EP, dtype=jnp.int32)[:, None, None], flat.shape)
    inverse = jnp.full((N_EP, EXPERTS * CAP), TOK_EP, jnp.int32)
    inverse = inverse.at[block_index.reshape(-1), flat.reshape(-1)].set(owner.reshape(-1))
    inverse = inverse.reshape(N_EP, EXPERTS, CAP)

    def one_expert(expert):
        local = lax.dynamic_index_in_dim(inverse, expert, 1, keepdims=False)
        valid = (local < TOK_EP).reshape(-1)[:, None]
        rows = (jnp.arange(N_EP, dtype=jnp.int32)[:, None] * TOK_EP + jnp.minimum(local, TOK_EP - 1)).reshape(-1)
        zero_value = jnp.zeros((), layer_input.dtype)
        inputs = jnp.where(valid, jnp.take(layer_input, rows, axis=0), zero_value)
        grads = jnp.where(valid, jnp.take(out_grad, rows, axis=0), zero_value)
        gate_matrix = lax.dynamic_index_in_dim(gate_weight, expert, 0, keepdims=False)
        up_matrix = lax.dynamic_index_in_dim(up_weight, expert, 0, keepdims=False)
        down_matrix = lax.dynamic_index_in_dim(down_weight, expert, 0, keepdims=False)
        return expert_rows(gate_matrix, up_matrix, down_matrix, inputs, grads)

    returned = lax.map(one_expert, jnp.arange(EXPERTS, dtype=jnp.int32))
    returned = returned.reshape(EXPERTS, N_EP, CAP, D)
    picked = returned[blocks, block_index, position]
    shares = gate_share.reshape(N_EP, TOK_EP, TOP)[..., None]
    combined = jnp.sum(picked.astype(jnp.float32) * shares, axis=2)
    return combined.reshape(TOKENS, D).astype(jnp.bfloat16)
```

```python
import jax
import jax.numpy as jnp
from jax import lax
from jax.experimental import pallas as pl
from jax.experimental.pallas import tpu as pltpu
from jax.sharding import PartitionSpec as P

BF = jnp.bfloat16
F32 = jnp.float32
SIDE = 4
TP = SIDE * SIDE
CHUNKS = 2
ROWS_BY_ROWS = (((1,), (1,)), ((), ()))
COLS_BY_COLS = (((0,), (0,)), ((), ()))


def flat_slots(routes, experts, capacity):
    tokens = routes.shape[1]
    first, second = routes[0:1, :], routes[1:2, :]
    expert = lax.broadcasted_iota(jnp.int32, (experts, tokens), 0)
    in_first, in_second = expert == first, expert == second
    named = jnp.where(in_first | in_second, 1.0, 0.0).astype(BF)
    earlier = lax.broadcasted_iota(jnp.int32, (tokens, tokens), 0)
    later = lax.broadcasted_iota(jnp.int32, (tokens, tokens), 1)
    before = jnp.dot(named, jnp.where(earlier < later, 1.0, 0.0).astype(BF), preferred_element_type=F32)
    place_first = jnp.sum(jnp.where(in_first, before, 0.0), axis=0, keepdims=True)
    place_second = jnp.sum(jnp.where(in_second, before, 0.0), axis=0, keepdims=True)
    return (
        first * capacity + place_first.astype(jnp.int32),
        second * capacity + place_second.astype(jnp.int32),
    )


def dispatch_body(routes, inputs, grads, to_x, *to_g):
    experts, capacity, _ = to_x.shape
    tokens = inputs.shape[0]
    first, second = flat_slots(routes[...], experts, capacity)
    slot = lax.broadcasted_iota(jnp.int32, (experts * capacity, tokens), 0)
    pick = jnp.where((slot == first) | (slot == second), 1.0, 0.0).astype(BF)
    rows = jnp.dot(pick, inputs[...], preferred_element_type=F32).astype(BF)
    for e in range(experts):
        to_x[e] = rows[e * capacity : (e + 1) * capacity]
    rows = jnp.dot(pick, grads[...], preferred_element_type=F32).astype(BF)
    part = capacity // len(to_g)
    for e in range(experts):
        for h, ref in enumerate(to_g):
            ref[e] = rows[e * capacity + h * part : e * capacity + (h + 1) * part]


def combine_body(routes, shares, *refs):
    backs, out = refs[:-1], refs[-1]
    experts, part, _ = backs[0].shape
    capacity = part * len(backs)
    tokens = out.shape[0]
    first, second = flat_slots(routes[...], experts, capacity)
    slot = lax.broadcasted_iota(jnp.int32, (experts * capacity, tokens), 0)
    share = jnp.concatenate([shares[...], jnp.zeros((6, tokens), F32)], axis=0).T
    back = jnp.concatenate([ref[e] for e in range(experts) for ref in backs], axis=0)
    one = lax.dot_general(
        jnp.where(slot == first, 1.0, 0.0).astype(BF), back, COLS_BY_COLS, preferred_element_type=F32
    )
    two = lax.dot_general(
        jnp.where(slot == second, 1.0, 0.0).astype(BF), back, COLS_BY_COLS, preferred_element_type=F32
    )
    out[...] = (one * share[:, 0:1] + two * share[:, 1:2]).astype(out.dtype)


def acts_body(x, gate, up, out):
    pieces = x.shape[0]
    left = jnp.concatenate([x[i] for i in range(pieces)], axis=1)
    right = jnp.concatenate([gate[...], up[...]], axis=1)
    part = jnp.dot(left, right, preferred_element_type=F32)

    @pl.when(pl.program_id(0) == 0)
    def _():
        out[...] = part

    @pl.when(pl.program_id(0) != 0)
    def _():
        out[...] += part


def hidden_body(g, down, acts, out, total):
    pieces = g.shape[0]
    left = jnp.concatenate([g[i] for i in range(pieces)], axis=1)
    part = lax.dot_general(left, down[...], ROWS_BY_ROWS, preferred_element_type=F32)
    step = pl.program_id(0)

    @pl.when(step == 0)
    def _():
        total[...] = part

    @pl.when(step != 0)
    def _():
        total[...] += part

    @pl.when(step == pl.num_programs(0) - 1)
    def _():
        width = total.shape[1]
        blocks, part_rows = acts.shape[0], acts.shape[2]
        for b in range(blocks):
            rows = slice(b * part_rows, (b + 1) * part_rows)
            gate = acts[b, 0, :, :width]
            up = acts[b, 0, :, width:]
            hidden = total[rows, :]
            sigma = jax.nn.sigmoid(gate)
            slope = sigma * (1.0 + gate * (1.0 - sigma))
            out[rows, :width] = (hidden * up * slope).astype(BF)
            out[rows, width:] = (hidden * gate * sigma).astype(BF)


def partial_body(order, grads, gate, up, out_a, out_b):
    right = jnp.concatenate([gate[...], up[...]], axis=1)
    part = lax.dot_general(grads[...], right, ROWS_BY_ROWS, preferred_element_type=F32).astype(BF)
    half = part.shape[0] // 2
    out_a[0, 0] = part[:half]
    out_b[0, 0] = part[half:]


def z_shift(by):
    return [(z * SIDE + y, (z + by) % SIDE * SIDE + y) for z in range(SIDE) for y in range(SIDE)]


def y_shift(by):
    return [(z * SIDE + y, z * SIDE + (y + by) % SIDE) for z in range(SIDE) for y in range(SIDE)]


def ring_sum(parts, shift):
    half = parts.shape[1] // 2
    far_up = lax.ppermute(parts[2, :half], "tp", shift(1))
    far_down = lax.ppermute(parts[2, half:], "tp", shift(-1))
    ahead = jnp.concatenate(
        [(parts[1, :half].astype(F32) + far_up.astype(F32)).astype(BF), parts[1, half:]], axis=0
    )
    behind = jnp.concatenate(
        [parts[3, :half], (parts[3, half:].astype(F32) + far_down.astype(F32)).astype(BF)], axis=0
    )
    from_below = lax.ppermute(ahead, "tp", shift(1))
    from_above = lax.ppermute(behind, "tp", shift(-1))
    return parts[0].astype(F32) + from_below.astype(F32) + from_above.astype(F32)


def local(layer_input, out_grad, route, gate_share, gate_weight, up_weight, down_weight):
    experts = lax.axis_size("ep")
    tokens, width = layer_input.shape
    choose = route.shape[1]
    capacity = tokens * choose * 3 // (2 * experts)
    part = capacity // CHUNKS
    rows = experts * part
    gate_matrix, up_matrix, down_matrix = gate_weight[0], up_weight[0], down_weight[0]
    features, units = gate_matrix.shape
    routes, shares = route.T, gate_share.T

    sent = pl.pallas_call(
        dispatch_body,
        out_shape=[jax.ShapeDtypeStruct((experts, capacity, width), BF)]
        + [jax.ShapeDtypeStruct((experts, part, width), BF)] * CHUNKS,
        name="dispatch",
    )(routes, layer_input, out_grad)
    got = [lax.all_to_all(s, "ep", split_axis=0, concat_axis=0, tiled=True) for s in sent]
    all_x = lax.all_gather(got[0].reshape(experts * capacity, width), "tp", axis=0, tiled=False)

    step = 2
    acts = pl.pallas_call(
        acts_body,
        grid=(TP // step,),
        in_specs=[
            pl.BlockSpec((step, experts * capacity, width), lambda k: (k, 0, 0)),
            pl.BlockSpec((step * width, units), lambda k: (k, 0)),
            pl.BlockSpec((step * width, units), lambda k: (k, 0)),
        ],
        out_specs=pl.BlockSpec((experts * capacity, 2 * units), lambda k: (0, 0)),
        out_shape=jax.ShapeDtypeStruct((experts * capacity, 2 * units), F32),
        name="acts",
    )(all_x, gate_matrix, up_matrix)
    acts = acts.reshape(experts, CHUNKS, part, 2 * units)

    me = lax.axis_index("tp")
    ahead = jnp.arange(TP, dtype=jnp.int32)
    order = (me // SIDE + ahead // SIDE) % SIDE * SIDE + (me % SIDE + ahead % SIDE) % SIDE

    backs = []
    for h in range(CHUNKS):
        all_g = lax.all_gather(got[1 + h].reshape(rows, width), "tp", axis=0, tiled=False)
        grads = pl.pallas_call(
            hidden_body,
            grid=(TP // step,),
            in_specs=[
                pl.BlockSpec((step, rows, width), lambda k: (k, 0, 0)),
                pl.BlockSpec((units, step * width), lambda k: (0, k)),
                pl.BlockSpec((experts, 1, part, 2 * units), lambda k, h=h: (0, h, 0, 0)),
            ],
            out_specs=pl.BlockSpec((rows, 2 * units), lambda k: (0, 0)),
            out_shape=jax.ShapeDtypeStruct((rows, 2 * units), BF),
            scratch_shapes=[pltpu.VMEM((rows, units), F32)],
            name="hidden",
        )(all_g, down_matrix, acts)
        part_a, part_b = pl.pallas_call(
            partial_body,
            grid_spec=pltpu.PrefetchScalarGridSpec(
                num_scalar_prefetch=1,
                grid=(TP,),
                in_specs=[
                    pl.BlockSpec((rows, 2 * units), lambda k, order: (0, 0)),
                    pl.BlockSpec((width, units), lambda k, order: (order[k], 0)),
                    pl.BlockSpec((width, units), lambda k, order: (order[k], 0)),
                ],
                out_specs=[
                    pl.BlockSpec((1, 1, rows // 2, width), lambda k, order: (k // SIDE, k % SIDE, 0, 0)),
                    pl.BlockSpec((1, 1, rows // 2, width), lambda k, order: (k % SIDE, k // SIDE, 0, 0)),
                ],
            ),
            out_shape=[jax.ShapeDtypeStruct((SIDE, SIDE, rows // 2, width), BF)] * 2,
            name="partial",
        )(order, grads, gate_matrix, up_matrix)
        sum_a = ring_sum(ring_sum(part_a, z_shift).astype(BF), y_shift)
        sum_b = ring_sum(ring_sum(part_b, y_shift).astype(BF), z_shift)
        summed = jnp.concatenate([sum_a, sum_b], axis=0).astype(BF).reshape(experts, part, width)
        backs.append(lax.all_to_all(summed, "ep", split_axis=0, concat_axis=0, tiled=True))

    return pl.pallas_call(
        combine_body,
        out_shape=jax.ShapeDtypeStruct((tokens, width), BF),
        name="combine",
    )(routes, shares, *backs)


def solution(mesh):
    return jax.shard_map(
        local,
        mesh=mesh,
        in_specs=(
            P("ep", "tp"),
            P("ep", "tp"),
            P("ep", None),
            P("ep", None),
            P("ep", None, "tp"),
            P("ep", None, "tp"),
            P("ep", "tp", None),
        ),
        out_specs=P("ep", "tp"),
        check_vma=False,
    )
```

```python
import jax
import jax.numpy as jnp
from jax import lax
from jax.experimental import pallas as pl
from jax.experimental.pallas import tpu as pltpu
from jax.sharding import PartitionSpec as P

BF = jnp.bfloat16
F32 = jnp.float32
SIDE = 4
TP = SIDE * SIDE
CHUNKS = 2
COLS_BY_COLS = (((0,), (0,)), ((), ()))


def flat_slots(routes, experts, capacity):
    tokens = routes.shape[1]
    first, second = routes[0:1, :], routes[1:2, :]
    expert = lax.broadcasted_iota(jnp.int32, (experts, tokens), 0)
    in_first, in_second = expert == first, expert == second
    named = jnp.where(in_first | in_second, 1.0, 0.0).astype(BF)
    earlier = lax.broadcasted_iota(jnp.int32, (tokens, tokens), 0)
    later = lax.broadcasted_iota(jnp.int32, (tokens, tokens), 1)
    before = jnp.dot(named, jnp.where(earlier < later, 1.0, 0.0).astype(BF), preferred_element_type=F32)
    place_first = jnp.sum(jnp.where(in_first, before, 0.0), axis=0, keepdims=True)
    place_second = jnp.sum(jnp.where(in_second, before, 0.0), axis=0, keepdims=True)
    return (
        first * capacity + place_first.astype(jnp.int32),
        second * capacity + place_second.astype(jnp.int32),
    )


def dispatch_body(routes, inputs, grads, out):
    experts, both, _ = out.shape
    capacity = both // 2
    tokens = inputs.shape[0]
    first, second = flat_slots(routes[...], experts, capacity)
    slot = lax.broadcasted_iota(jnp.int32, (experts * capacity, tokens), 0)
    pick = jnp.where((slot == first) | (slot == second), 1.0, 0.0).astype(BF)
    for at, source in ((0, inputs), (capacity, grads)):
        rows = jnp.dot(pick, source[...], preferred_element_type=F32).astype(BF)
        for e in range(experts):
            out[e, at : at + capacity] = rows[e * capacity : (e + 1) * capacity]


def combine_body(routes, shares, *refs):
    backs, out = refs[:-1], refs[-1]
    experts, part, _ = backs[0].shape
    capacity = part * len(backs)
    tokens = out.shape[0]
    first, second = flat_slots(routes[...], experts, capacity)
    slot = lax.broadcasted_iota(jnp.int32, (experts * capacity, tokens), 0)
    share = jnp.concatenate([shares[...], jnp.zeros((6, tokens), F32)], axis=0).T
    back = jnp.concatenate([ref[e] for e in range(experts) for ref in backs], axis=0)
    one = lax.dot_general(
        jnp.where(slot == first, 1.0, 0.0).astype(BF), back, COLS_BY_COLS, preferred_element_type=F32
    )
    two = lax.dot_general(
        jnp.where(slot == second, 1.0, 0.0).astype(BF), back, COLS_BY_COLS, preferred_element_type=F32
    )
    out[...] = (one * share[:, 0:1] + two * share[:, 1:2]).astype(out.dtype)


def acts_body(order, *refs):
    pieces, (gate, up, gate_out, up_out, rows_by_features) = refs[:-5], refs[-5:]
    per_half = len(pieces) // 2
    width = pieces[0].shape[-1]

    @pl.when(pl.program_id(0) == 0)
    def _():
        for half in range(2):
            own, below, above, far_low, far_high = pieces[half * per_half : (half + 1) * per_half]
            count = own.shape[1]
            rows = slice(half * count, (half + 1) * count)
            for s in range(SIDE):
                for f in range(SIDE):
                    if s < 3:
                        value = (own, below, above)[s][f]
                    else:
                        value = (far_low if f < 2 else far_high)[f % 2]
                    block = order[(half * SIDE + s) * SIDE + f]
                    rows_by_features[rows, pl.ds(pl.multiple_of(block * width, width), width)] = value

    right = jnp.concatenate([gate[...], up[...]], axis=1)
    both = jnp.dot(rows_by_features[...], right, preferred_element_type=F32)
    strip = gate.shape[1]
    gate_out[...] = both[:, :strip]
    up_out[...] = both[:, strip:]


def hidden_body(g, down, gate_act, up_act, out, left, total):
    pieces, blocks, part_rows, width = g.shape
    for i in range(pieces):
        for b in range(blocks):
            left[b * part_rows : (b + 1) * part_rows, i * width : (i + 1) * width] = g[i, b]
    part = jnp.dot(left[...], down[...], preferred_element_type=F32)
    step = pl.program_id(0)

    @pl.when(step == 0)
    def _():
        total[...] = part

    @pl.when(step != 0)
    def _():
        total[...] += part

    @pl.when(step == pl.num_programs(0) - 1)
    def _():
        units = total.shape[1]
        for b in range(blocks):
            rows = slice(b * part_rows, (b + 1) * part_rows)
            gate = gate_act[b, 0]
            hidden = total[rows, :]
            sigma = jax.nn.sigmoid(gate)
            slope = sigma * (1.0 + gate * (1.0 - sigma))
            out[rows, :units] = (hidden * up_act[b, 0] * slope).astype(BF)
            out[rows, units:] = (hidden * gate * sigma).astype(BF)


def partial_body(order, grads, *refs):
    out = refs[-1]
    count = (len(refs) - 1) // 2
    columns = [jnp.concatenate([refs[2 * i][...], refs[2 * i + 1][...]], axis=0) for i in range(count)]
    right = jnp.concatenate(columns, axis=1)
    part = jnp.dot(grads[...], right, preferred_element_type=F32).astype(BF)
    width = out.shape[-1]
    for i in range(count):
        out[0, i] = part[:, i * width : (i + 1) * width]


def z_shift(by):
    return [(z * SIDE + y, (z + by) % SIDE * SIDE + y) for z in range(SIDE) for y in range(SIDE)]


def y_shift(by):
    return [(z * SIDE + y, z * SIDE + (y + by) % SIDE) for z in range(SIDE) for y in range(SIDE)]


def ring_gather(x, shift):
    half = x.shape[0] // 2
    below = lax.ppermute(x, "tp", shift(1))
    above = lax.ppermute(x, "tp", shift(-1))
    far_low = lax.ppermute(below[:half], "tp", shift(1))
    far_high = lax.ppermute(above[half:], "tp", shift(-1))
    return [x, below, above, far_low, far_high]


def plane_gather(x, first, second):
    rows, width = x.shape
    line = jnp.concatenate(ring_gather(x, first), axis=0)
    return [piece.reshape(-1, rows, width) for piece in ring_gather(line, second)]


def ring_sum(own, ahead, far, behind, shift):
    half = far.shape[0] // 2
    far_up = lax.ppermute(far[:half].astype(BF), "tp", shift(1))
    far_down = lax.ppermute(far[half:].astype(BF), "tp", shift(-1))
    ahead, behind = ahead.astype(F32), behind.astype(F32)
    up = jnp.concatenate([ahead[:half] + far_up.astype(F32), ahead[half:]], axis=0).astype(BF)
    down = jnp.concatenate([behind[:half], behind[half:] + far_down.astype(F32)], axis=0).astype(BF)
    from_below = lax.ppermute(up, "tp", shift(1))
    from_above = lax.ppermute(down, "tp", shift(-1))
    return own.astype(F32) + from_below.astype(F32) + from_above.astype(F32)


def local(layer_input, out_grad, route, gate_share, gate_weight, up_weight, down_weight):
    experts = lax.axis_size("ep")
    tokens, width = layer_input.shape
    choose = route.shape[1]
    capacity = tokens * choose * 3 // (2 * experts)
    slots = experts * capacity
    part = capacity // CHUNKS
    rows = experts * part
    gate_matrix, up_matrix, down_matrix = gate_weight[0], up_weight[0], down_weight[0]
    features, units = gate_matrix.shape
    routes, shares = route.T, gate_share.T

    me = lax.axis_index("tp")
    z, y = me // SIDE, me % SIDE
    away = jnp.array([0, SIDE - 1, 1, 2], jnp.int32)
    steps = jnp.arange(SIDE, dtype=jnp.int32)

    def plane(in_z, in_y):
        return ((z + in_z) % SIDE * SIDE + (y + in_y) % SIDE).astype(jnp.int32)

    gathered_order = jnp.stack(
        [plane(away[None, :], away[:, None]), plane(away[:, None], away[None, :])]
    ).reshape(-1)
    summed_order = [plane(steps[:, None], steps[None, :]), plane(steps[None, :], steps[:, None])]

    sent = pl.pallas_call(
        dispatch_body,
        out_shape=jax.ShapeDtypeStruct((experts, 2 * capacity, width), BF),
        name="dispatch",
    )(routes, layer_input, out_grad)
    got = lax.all_to_all(sent, "ep", split_axis=0, concat_axis=0, tiled=True)
    all_g = lax.all_gather(got[:, capacity:].reshape(slots, width), "tp", axis=0, tiled=False)
    all_g = all_g.reshape(TP, experts, capacity, width)
    low = got[: experts // 2, :capacity].reshape(slots // 2, width)
    high = got[experts // 2 :, :capacity].reshape(slots // 2, width)
    pieces = plane_gather(low, z_shift, y_shift) + plane_gather(high, y_shift, z_shift)

    strip = 128
    whole = [pl.BlockSpec(p.shape, lambda n, order: (0, 0, 0)) for p in pieces]
    acts = pl.pallas_call(
        acts_body,
        grid_spec=pltpu.PrefetchScalarGridSpec(
            num_scalar_prefetch=1,
            grid=(units // strip,),
            in_specs=whole + [pl.BlockSpec((features, strip), lambda n, order: (0, n))] * 2,
            out_specs=[pl.BlockSpec((slots, strip), lambda n, order: (0, n))] * 2,
            scratch_shapes=[pltpu.VMEM((slots, features), BF)],
        ),
        out_shape=[jax.ShapeDtypeStruct((slots, units), F32)] * 2,
        name="acts",
    )(gathered_order, *pieces, gate_matrix, up_matrix)
    acts = [a.reshape(experts, CHUNKS, part, units) for a in acts]
    gate_turned, up_turned, down_turned = lax.optimization_barrier((gate_matrix.T, up_matrix.T, down_matrix.T))

    def partial(grads, order):
        groups = order.shape[0]
        at_once = 2
        per_group = SIDE // at_once

        def column(i):
            return pl.BlockSpec((units, width), lambda k, order, i=i: (0, order[k * at_once + i]))

        specs, weights = [], []
        for i in range(at_once):
            specs += [column(i), column(i)]
            weights += [gate_turned, up_turned]
        return pl.pallas_call(
            partial_body,
            grid_spec=pltpu.PrefetchScalarGridSpec(
                num_scalar_prefetch=1,
                grid=(groups * per_group,),
                in_specs=[pl.BlockSpec((rows, 2 * units), lambda k, order: (0, 0))] + specs,
                out_specs=pl.BlockSpec(
                    (1, at_once, rows, width), lambda k, order: (k // per_group, k % per_group, 0, 0)
                ),
            ),
            out_shape=jax.ShapeDtypeStruct((groups, SIDE, rows, width), BF),
            name="partial",
        )(order.reshape(-1), grads, *weights)

    span = 4
    backs = []
    for h in range(CHUNKS):
        grads = pl.pallas_call(
            hidden_body,
            grid=(TP // span,),
            in_specs=[
                pl.BlockSpec((span, experts, part, width), lambda k, h=h: (k, 0, h, 0)),
                pl.BlockSpec((span * width, units), lambda k: (k, 0)),
                pl.BlockSpec((experts, 1, part, units), lambda k, h=h: (0, h, 0, 0)),
                pl.BlockSpec((experts, 1, part, units), lambda k, h=h: (0, h, 0, 0)),
            ],
            out_specs=pl.BlockSpec((rows, 2 * units), lambda k: (0, 0)),
            out_shape=jax.ShapeDtypeStruct((rows, 2 * units), BF),
            scratch_shapes=[pltpu.VMEM((rows, span * width), BF), pltpu.VMEM((rows, units), F32)],
            name="hidden",
        )(all_g, down_turned, *acts)
        order = summed_order[h]
        far = partial(grads, order[2:3])[0]
        near = partial(grads, order[1::2])
        if h + 1 < CHUNKS:
            far, near, *acts = lax.optimization_barrier((far, near, *acts))
        own = partial(grads, order[0:1])[0]
        first, second = (z_shift, y_shift) if h == 0 else (y_shift, z_shift)
        line = ring_sum(own, near[0], far, near[1], first)
        summed = ring_sum(line[0], line[1], line[2], line[3], second).astype(BF)
        summed = summed.reshape(experts, part, width)
        backs.append(lax.all_to_all(summed, "ep", split_axis=0, concat_axis=0, tiled=True))

    return pl.pallas_call(
        combine_body,
        out_shape=jax.ShapeDtypeStruct((tokens, width), BF),
        name="combine",
    )(routes, shares, *backs)


def solution(mesh):
    return jax.shard_map(
        local,
        mesh=mesh,
        in_specs=(
            P("ep", "tp"),
            P("ep", "tp"),
            P("ep", None),
            P("ep", None),
            P("ep", None, "tp"),
            P("ep", None, "tp"),
            P("ep", "tp", None),
        ),
        out_specs=P("ep", "tp"),
        check_vma=False,
    )
```

```python
import functools

import jax
import jax.numpy as jnp
from jax import lax
from jax.experimental import pallas as pl
from jax.experimental.pallas import tpu as pltpu
from jax.sharding import PartitionSpec as P


BF = jnp.bfloat16
F32 = jnp.float32
SIDE = 4
TP = SIDE * SIDE
COLS_BY_COLS = (((0,), (0,)), ((), ()))


def flat_slots(routes, experts, capacity):
    tokens = routes.shape[1]
    first, second = routes[0:1, :], routes[1:2, :]
    expert = lax.broadcasted_iota(jnp.int32, (experts, tokens), 0)
    in_first, in_second = expert == first, expert == second
    named = jnp.where(in_first | in_second, 1.0, 0.0).astype(BF)
    earlier = lax.broadcasted_iota(jnp.int32, (tokens, tokens), 0)
    later = lax.broadcasted_iota(jnp.int32, (tokens, tokens), 1)
    before = jnp.dot(named, jnp.where(earlier < later, 1.0, 0.0).astype(BF), preferred_element_type=F32)
    place_first = jnp.sum(jnp.where(in_first, before, 0.0), axis=0, keepdims=True)
    place_second = jnp.sum(jnp.where(in_second, before, 0.0), axis=0, keepdims=True)
    return (
        first * capacity + place_first.astype(jnp.int32),
        second * capacity + place_second.astype(jnp.int32),
    )


def dispatch_body(routes, inputs, grads, out):
    experts, both, _ = out.shape
    capacity = both // 2
    tokens = inputs.shape[0]
    first, second = flat_slots(routes[...], experts, capacity)
    slot = lax.broadcasted_iota(jnp.int32, (experts * capacity, tokens), 0)
    pick = jnp.where((slot == first) | (slot == second), 1.0, 0.0).astype(BF)
    for at, source in ((0, inputs), (capacity, grads)):
        rows = jnp.dot(pick, source[...], preferred_element_type=F32).astype(BF)
        for e in range(experts):
            out[e, at : at + capacity] = rows[e * capacity : (e + 1) * capacity]


def combine_body(routes, shares, *refs):
    backs, out = refs[:-1], refs[-1]
    experts, part, _ = backs[0].shape
    capacity = part * len(backs)
    tokens = out.shape[0]
    first, second = flat_slots(routes[...], experts, capacity)
    slot = lax.broadcasted_iota(jnp.int32, (experts * capacity, tokens), 0)
    share = jnp.concatenate([shares[...], jnp.zeros((6, tokens), F32)], axis=0).T
    back = jnp.concatenate([ref[e] for e in range(experts) for ref in backs], axis=0)
    one = lax.dot_general(
        jnp.where(slot == first, 1.0, 0.0).astype(BF), back, COLS_BY_COLS, preferred_element_type=F32
    )
    two = lax.dot_general(
        jnp.where(slot == second, 1.0, 0.0).astype(BF), back, COLS_BY_COLS, preferred_element_type=F32
    )
    out[...] = (one * share[:, 0:1] + two * share[:, 1:2]).astype(out.dtype)


def turn_body(gate, up, down, wide, tall):
    units = gate.shape[1]
    wide[0, :units] = gate[...].T
    wide[0, units:] = up[...].T
    tall[0] = down[...].T


def acts_body(order, *refs, first, count):
    gate_out, up_out, rows_by_features = refs[-3:]
    before = refs[-5:-3] if first > 0 else ()
    ins = refs[: -3 - len(before)]
    pieces, (gate, up) = ins[:-2], ins[-2:]
    per_half = len(pieces) // 2
    width = pieces[0].shape[-1]
    unit = gate.shape[-1]

    @pl.when(pl.program_id(0) == 0)
    def _():
        for half in range(2):
            blocks = [p[i] for p in pieces[half * per_half : (half + 1) * per_half] for i in range(p.shape[0])]
            for s in range(count):
                for f in range(SIDE):
                    rows_by_features[half * count + s, :, f * width : (f + 1) * width] = blocks[s * SIDE + f]

    for half in range(2):
        total = None
        for s in range(count):
            named = [order[(half * SIDE + first + s) * SIDE + f] for f in range(SIDE)]
            right = jnp.concatenate([jnp.concatenate([gate[t], up[t]], axis=1) for t in named], axis=0)
            part = jnp.dot(rows_by_features[half * count + s], right, preferred_element_type=F32)
            total = part if total is None else total + part
        blocks = gate_out.shape[0] // 2
        here = slice(half * blocks, (half + 1) * blocks)
        shape = (blocks, gate_out.shape[1], unit)
        gate_sum, up_sum = total[:, :unit].reshape(shape), total[:, unit:].reshape(shape)
        if before:
            gate_sum = gate_sum + before[0][here]
            up_sum = up_sum + before[1][here]
        gate_out[here] = gate_sum
        up_out[here] = up_sum


def expert_body(order, g, tall, gate_act, up_act, *refs):
    members = len(refs) - SIDE - 5
    wide, outs = refs[:members], refs[members:-5]
    left, total, for_gate, for_up, grads = refs[-5:]
    pieces, blocks, part_rows, width = g.shape
    units = total.shape[1]
    step = pl.program_id(0)
    deep = TP // pieces

    @pl.when(step < deep)
    def _():
        for i in range(pieces):
            for b in range(blocks):
                left[b * part_rows : (b + 1) * part_rows, i * width : (i + 1) * width] = g[i, b]
        part = jnp.dot(left[...], tall[...].reshape(pieces * width, units), preferred_element_type=F32)

        @pl.when(step == 0)
        def _():
            total[...] = part

        @pl.when(step != 0)
        def _():
            total[...] += part

        count = gate_act.shape[0] * part_rows
        gate = gate_act[...].reshape(count, units)
        sigma = jax.nn.sigmoid(gate)
        here = pl.ds(pl.multiple_of(step * count, count), count)
        for_gate[here] = up_act[...].reshape(count, units) * (sigma * (1.0 + gate * (1.0 - sigma)))
        for_up[here] = gate * sigma

    @pl.when(step == deep)
    def _():
        grads[:, :units] = (total[...] * for_gate[...]).astype(BF)
        grads[:, units:] = (total[...] * for_up[...]).astype(BF)

    @pl.when(step >= deep)
    def _():
        right = jnp.concatenate([w[0] for w in wide], axis=1)
        part = jnp.dot(grads[...], right, preferred_element_type=F32).astype(BF)
        per_out = SIDE // members
        for at, out in enumerate(outs):

            @pl.when((step - deep) // per_out == at)
            def _():
                for i in range(members):
                    out[i] = part[:, i * width : (i + 1) * width]


def vmem(mebibytes):
    return pltpu.CompilerParams(vmem_limit_bytes=mebibytes << 20)


def in_hbm(*arrays):
    return [pltpu.with_memory_space_constraint(a, pltpu.HBM) for a in arrays]


def z_shift(by):
    return [(z * SIDE + y, (z + by) % SIDE * SIDE + y) for z in range(SIDE) for y in range(SIDE)]


def y_shift(by):
    return [(z * SIDE + y, z * SIDE + (y + by) % SIDE) for z in range(SIDE) for y in range(SIDE)]


def shifted(x, shift, by):
    return lax.ppermute(x, "tp", shift(by))


def ring_gather(x, shift):
    half = x.shape[0] // 2
    below = shifted(x, shift, 1)
    above = shifted(x, shift, 3)
    far_low = shifted(below[:half], shift, 1)
    far_high = shifted(above[half:], shift, 3)
    return [x, below, above, far_low, far_high]


def plane_gather(x, first, second):
    rows, width = x.shape
    line = jnp.concatenate(ring_gather(x, first), axis=0)
    return [piece.reshape(-1, rows, width) for piece in ring_gather(line, second)]


def ring_sum(far, ahead, behind, own, shift):
    total = own.astype(F32)
    for by, part in ((2, far), (1, ahead), (3, behind)):
        total = total + shifted(part.astype(BF), shift, by).astype(F32)
    return total


def body(layer_input, out_grad, route, gate_share, gate_weight, up_weight, down_weight):
    experts = lax.axis_size("ep")
    tokens, width = layer_input.shape
    choose = route.shape[1]
    capacity = tokens * choose * 3 // (2 * experts)
    slots = experts * capacity
    parts = (2 * capacity // 3, capacity // 3)
    gate_matrix, up_matrix, down_matrix = gate_weight[0], up_weight[0], down_weight[0]
    _, units = gate_matrix.shape
    routes, shares = route.T, gate_share.T

    me = lax.axis_index("tp")
    z, y = me // SIDE, me % SIDE
    away = jnp.array([0, SIDE - 1, 1, 2], jnp.int32)
    steps = jnp.arange(SIDE, dtype=jnp.int32)

    def plane(in_z, in_y):
        return ((z + in_z) % SIDE * SIDE + (y + in_y) % SIDE).astype(jnp.int32)

    gathered_order = jnp.stack(
        [plane(away[None, :], away[:, None]), plane(away[:, None], away[None, :])]
    ).reshape(-1)
    summed_order = [plane(steps[:, None], steps[None, :]), plane(steps[None, :], steps[:, None])]

    sent = pl.pallas_call(
        dispatch_body,
        out_shape=jax.ShapeDtypeStruct((experts, 2 * capacity, width), BF),
        name="dispatch",
        compiler_params=vmem(16),
    )(routes, layer_input, out_grad)
    got = lax.all_to_all(sent, "ep", split_axis=0, concat_axis=0, tiled=True)
    all_g = lax.all_gather(got[:, capacity:].reshape(slots, width), "tp", axis=0, tiled=False)
    all_g = all_g.reshape(TP, experts, capacity, width)
    low = got[: experts // 2, :capacity].reshape(slots // 2, width)
    high = got[experts // 2 :, :capacity].reshape(slots // 2, width)
    pieces = plane_gather(low, z_shift, y_shift) + plane_gather(high, y_shift, z_shift)

    wide, tall = pl.pallas_call(
        turn_body,
        grid=(TP,),
        in_specs=[
            pl.BlockSpec((width, units), lambda k: (k, 0)),
            pl.BlockSpec((width, units), lambda k: (k, 0)),
            pl.BlockSpec((units, width), lambda k: (0, k)),
        ],
        out_specs=[
            pl.BlockSpec((1, 2 * units, width), lambda k: (k, 0, 0)),
            pl.BlockSpec((1, width, units), lambda k: (k, 0, 0)),
        ],
        out_shape=[
            jax.ShapeDtypeStruct((TP, 2 * units, width), BF),
            jax.ShapeDtypeStruct((TP, width, units), BF),
        ],
        name="turn",
        compiler_params=vmem(16),
    )(*in_hbm(gate_matrix, up_matrix, down_matrix))

    strip = 128
    acts = []
    per_half = len(pieces) // 2
    for first, count in ((0, SIDE - 1), (SIDE - 1, 1)):
        which = slice(0, 3) if first == 0 else slice(3, 5)
        used = pieces[:per_half][which] + pieces[per_half:][which]
        column = pl.BlockSpec((experts, capacity, strip), lambda n, order: (0, 0, n))
        acts = pl.pallas_call(
            functools.partial(acts_body, first=first, count=count),
            grid_spec=pltpu.PrefetchScalarGridSpec(
                num_scalar_prefetch=1,
                grid=(units // strip,),
                in_specs=[pl.BlockSpec(p.shape, lambda n, order: (0, 0, 0)) for p in used]
                + [pl.BlockSpec((TP, width, strip), lambda n, order: (0, 0, n))] * 2
                + [column] * len(acts),
                out_specs=[column] * 2,
                scratch_shapes=[pltpu.VMEM((2 * count, slots // 2, SIDE * width), BF)],
            ),
            out_shape=[jax.ShapeDtypeStruct((experts, capacity, units), F32)] * 2,
            name="acts",
            compiler_params=vmem(40),
        )(
            gathered_order,
            *in_hbm(*used, gate_matrix.reshape(TP, width, units), up_matrix.reshape(TP, width, units)),
            *acts,
        )

    span = 4
    at_once = 2
    deep, per_out = TP // span, SIDE // at_once
    summed = []
    for h, part in enumerate(parts):
        start = sum(parts[:h]) // part
        rows = experts * part

        def wide_block(i):
            return lambda k, order: (order[jnp.maximum(k - deep, 0) * at_once + i], 0, 0)

        def out_block(at):
            return lambda k, order: (jnp.clip(k - deep - at * per_out, 0, per_out - 1), 0, 0)

        deep_step = lambda k: jnp.minimum(k, deep - 1)
        acts_block = pl.BlockSpec(
            (experts // deep, part, units), lambda k, order, start=start: (deep_step(k), start, 0)
        )
        outs = pl.pallas_call(
            expert_body,
            grid_spec=pltpu.PrefetchScalarGridSpec(
                num_scalar_prefetch=1,
                grid=(deep + SIDE * per_out,),
                in_specs=[
                    pl.BlockSpec(
                        (span, experts, part, width),
                        lambda k, order, start=start: (deep_step(k), 0, start, 0),
                    ),
                    pl.BlockSpec((span, width, units), lambda k, order: (deep_step(k), 0, 0)),
                    acts_block,
                    acts_block,
                ]
                + [pl.BlockSpec((1, 2 * units, width), wide_block(i)) for i in range(at_once)],
                out_specs=[pl.BlockSpec((at_once, rows, width), out_block(at)) for at in range(SIDE)],
                scratch_shapes=[pltpu.VMEM((rows, span * width), BF)]
                + [pltpu.VMEM((rows, units), F32)] * 3
                + [pltpu.VMEM((rows, 2 * units), BF)],
            ),
            out_shape=[jax.ShapeDtypeStruct((SIDE, rows, width), BF)] * SIDE,
            name="expert",
            compiler_params=vmem(40),
        )(
            summed_order[h][jnp.array([2, 1, 3, 0])].reshape(-1),
            *in_hbm(all_g, tall, *acts, *[wide] * at_once),
        )
        first, second = (z_shift, y_shift) if h == 0 else (y_shift, z_shift)
        line = ring_sum(*outs, first)
        mine = ring_sum(line[2], line[1], line[3], line[0], second)
        summed.append(mine.astype(BF).reshape(experts, part, width))
    backs = [
        lax.all_to_all(jnp.concatenate(summed, axis=1), "ep", split_axis=0, concat_axis=0, tiled=True)
    ]

    return pl.pallas_call(
        combine_body,
        out_shape=jax.ShapeDtypeStruct((tokens, width), BF),
        name="combine",
        compiler_params=vmem(16),
    )(routes, shares, *backs)


def solution(mesh):
    return jax.shard_map(
        body,
        mesh=mesh,
        in_specs=(
            P("ep", "tp"),
            P("ep", "tp"),
            P("ep", None),
            P("ep", None),
            P("ep", None, "tp"),
            P("ep", None, "tp"),
            P("ep", "tp", None),
        ),
        out_specs=P("ep", "tp"),
        check_vma=False,
    )
```

```python
import functools

import jax
import jax.numpy as jnp
import numpy as np
from jax import lax
from jax.experimental import pallas as pl
from jax.experimental.pallas import tpu as pltpu
from jax.sharding import PartitionSpec as P


BF = jnp.bfloat16
F32 = jnp.float32
SIDE = 4
TP = SIDE * SIDE
COLS_BY_COLS = (((0,), (0,)), ((), ()))


def flat_slots(routes, experts, capacity):
    tokens = routes.shape[1]
    first, second = routes[0:1, :], routes[1:2, :]
    expert = lax.broadcasted_iota(jnp.int32, (experts, tokens), 0)
    in_first, in_second = expert == first, expert == second
    named = jnp.where(in_first | in_second, 1.0, 0.0).astype(BF)
    earlier = lax.broadcasted_iota(jnp.int32, (tokens, tokens), 0)
    later = lax.broadcasted_iota(jnp.int32, (tokens, tokens), 1)
    before = jnp.dot(named, jnp.where(earlier < later, 1.0, 0.0).astype(BF), preferred_element_type=F32)
    place_first = jnp.sum(jnp.where(in_first, before, 0.0), axis=0, keepdims=True)
    place_second = jnp.sum(jnp.where(in_second, before, 0.0), axis=0, keepdims=True)
    return (
        first * capacity + place_first.astype(jnp.int32),
        second * capacity + place_second.astype(jnp.int32),
    )


def dispatch_body(routes, inputs, grads, out):
    experts, both, _ = out.shape
    capacity = both // 2
    tokens = inputs.shape[0]
    first, second = flat_slots(routes[...], experts, capacity)
    slot = lax.broadcasted_iota(jnp.int32, (experts * capacity, tokens), 0)
    pick = jnp.where((slot == first) | (slot == second), 1.0, 0.0).astype(BF)
    for at, source in ((0, inputs), (capacity, grads)):
        rows = jnp.dot(pick, source[...], preferred_element_type=F32).astype(BF)
        for e in range(experts):
            out[e, at : at + capacity] = rows[e * capacity : (e + 1) * capacity]


def combine_body(routes, shares, *refs):
    backs, out = refs[:-1], refs[-1]
    experts, part, _ = backs[0].shape
    capacity = part * len(backs)
    tokens = out.shape[0]
    first, second = flat_slots(routes[...], experts, capacity)
    slot = lax.broadcasted_iota(jnp.int32, (experts * capacity, tokens), 0)
    share = jnp.concatenate([shares[...], jnp.zeros((6, tokens), F32)], axis=0).T
    back = jnp.concatenate([ref[e] for e in range(experts) for ref in backs], axis=0)
    one = lax.dot_general(
        jnp.where(slot == first, 1.0, 0.0).astype(BF), back, COLS_BY_COLS, preferred_element_type=F32
    )
    two = lax.dot_general(
        jnp.where(slot == second, 1.0, 0.0).astype(BF), back, COLS_BY_COLS, preferred_element_type=F32
    )
    out[...] = (one * share[:, 0:1] + two * share[:, 1:2]).astype(out.dtype)


def turn_body(gate, up, down, wide, tall):
    units = gate.shape[1]
    wide[0, :units] = gate[...].T
    wide[0, units:] = up[...].T
    tall[0] = down[...].T


def acts_body(order, *refs, first, count):
    if first > 0:
        pieces, (before, gate, up, out, weights, rows, arrived, result, leaving) = refs[:-9], refs[-9:]
    else:
        pieces, (gate, up, out, weights, rows, arrived) = refs[:-6], refs[-6:]
        result, before = out, None
    per_half = len(pieces) // 2
    units = gate.shape[-1]
    width = gate.shape[1]

    def fetch(k):
        return [
            pltpu.make_async_copy(gate.at[order[k]], weights.at[k, :, :units], arrived.at[0, k]),
            pltpu.make_async_copy(up.at[order[k]], weights.at[k, :, units:], arrived.at[1, k]),
        ]

    lows = [SIDE * s + f for s in range(first, first + count) for f in range(SIDE)]
    highs = [SIDE * f + s for s in range(first, first + count) for f in range(SIDE)]
    for k in dict.fromkeys(lows + highs):
        for copy in fetch(k):
            copy.start()
    for half in range(2):
        blocks = [p.at[i] for p in pieces[half * per_half : (half + 1) * per_half] for i in range(p.shape[0])]
        for at, block in enumerate(blocks):
            s, f = at // SIDE, at % SIDE
            rows[half * count + s, :, f * width : (f + 1) * width] = block[...]

    for half in range(2):

        def ring(i, carry, half=half):
            s = first + i
            slots = [SIDE * s + f if half == 0 else SIDE * f + s for f in range(SIDE)]
            for f in range(SIDE):
                if half == 0 or (f >= SIDE - 1 if first == 0 else f < SIDE - 1):
                    for copy in fetch(slots[f]):
                        copy.wait()
            right = jnp.concatenate([weights[k] for k in slots], axis=0)
            part = jnp.dot(rows[half * count + i], right, preferred_element_type=F32)
            if before is not None:
                result[half] = before[half] + part
            else:

                @pl.when(i == 0)
                def _():
                    result[half] = part

                @pl.when(i != 0)
                def _():
                    result[half] += part

            return carry

        lax.fori_loop(0, count, ring, 0)
        if first > 0:
            pltpu.make_async_copy(result.at[half], out.at[half], leaving.at[half]).start()
    if first > 0:
        for half in range(2):
            pltpu.make_async_copy(result.at[half], out.at[half], leaving.at[half]).wait()


def expert_body(order, acts, g, tall, wide, *refs, start):
    outs = refs[:SIDE]
    left, downs, sides, held, total, grads, g_here, tall_here, wide_here, acts_here = refs[SIDE:]
    experts, part_rows, features = left.shape
    rows = experts * part_rows
    width = features // TP
    units = total.shape[1]
    deep = 4
    span = TP // deep

    def fetch_g(t, lanes):
        return pltpu.make_async_copy(g.at[t, :, start : start + part_rows, :], left.at[:, :, lanes], g_here.at[t])

    def fetch_tall(i, here):
        return pltpu.make_async_copy(tall.at[here], downs.at[here], tall_here.at[i])

    def fetch_wide(k):
        return pltpu.make_async_copy(wide.at[order[k]], sides.at[k], wide_here.at[k])

    fetch_acts = pltpu.make_async_copy(acts.at[:, start : start + part_rows, :], held, acts_here.at[0])
    for i in range(deep):
        for t in range(i * span, (i + 1) * span):
            fetch_g(t, slice(t * width, (t + 1) * width)).start()
        fetch_tall(i, slice(i * span, (i + 1) * span)).start()
    fetch_acts.start()
    for k in range(TP):
        fetch_wide(k).start()

    def deepen(i, carry):
        for j in range(span):
            t = i * span + j
            fetch_g(t, pl.ds(pl.multiple_of(t * width, width), width)).wait()
        here = pl.ds(i * span, span)
        fetch_tall(i, here).wait()
        step = span * width
        part = jnp.dot(
            left[:, :, pl.ds(pl.multiple_of(i * step, step), step)].reshape(rows, step),
            downs[here].reshape(step, units),
            preferred_element_type=F32,
        )

        @pl.when(i == 0)
        def _():
            total[...] = part

        @pl.when(i != 0)
        def _():
            total[...] += part

        return carry

    lax.fori_loop(0, deep, deepen, 0)
    fetch_acts.wait()

    def form(b, carry):
        here = pl.ds(pl.multiple_of(b * part_rows, part_rows), part_rows)
        gate, up = held[b, :, :units], held[b, :, units:]
        hidden = total[here]
        sigma = jax.nn.sigmoid(gate)
        slope = sigma * (1.0 + gate * (1.0 - sigma))
        grads[here, :units] = (hidden * up * slope).astype(BF)
        grads[here, units:] = (hidden * gate * sigma).astype(BF)
        return carry

    lax.fori_loop(0, experts, form, 0)

    def members(j, carry):
        k = 2 * j
        fetch_wide(k).wait()
        fetch_wide(k + 1).wait()
        right = jnp.concatenate([sides[k], sides[k + 1]], axis=1)
        part = jnp.dot(grads[...], right, preferred_element_type=F32).astype(BF)
        for f in range(SIDE):

            @pl.when(k // SIDE == f)
            def _():
                outs[f][k % SIDE] = part[:, :width]
                outs[f][k % SIDE + 1] = part[:, width:]

        return carry

    lax.fori_loop(0, TP // 2, members, 0)


def vmem(mebibytes):
    return pltpu.CompilerParams(vmem_limit_bytes=mebibytes << 20)


def in_hbm(*arrays):
    return [pltpu.with_memory_space_constraint(a, pltpu.HBM) for a in arrays]


def z_shift(by):
    return [(z * SIDE + y, (z + by) % SIDE * SIDE + y) for z in range(SIDE) for y in range(SIDE)]


def y_shift(by):
    return [(z * SIDE + y, z * SIDE + (y + by) % SIDE) for z in range(SIDE) for y in range(SIDE)]


def shifted(x, shift, by):
    return lax.ppermute(x, "tp", shift(by))


def ring_gather(x, shift):
    half = x.shape[0] // 2
    below = shifted(x, shift, 1)
    above = shifted(x, shift, 3)
    far_low = shifted(below[:half], shift, 1)
    far_high = shifted(above[half:], shift, 3)
    return [x, below, above, far_low, far_high]


def plane_gather(x, first, second):
    rows, width = x.shape
    line = jnp.concatenate(ring_gather(x, first), axis=0)
    return [piece.reshape(-1, rows, width) for piece in ring_gather(line, second)]


def ring_sum(far, ahead, behind, own, shift):
    total = own.astype(F32)
    for by, part in ((2, far), (1, ahead), (3, behind)):
        total = total + shifted(part.astype(BF), shift, by).astype(F32)
    return total


def body(layer_input, out_grad, route, gate_share, gate_weight, up_weight, down_weight):
    experts = lax.axis_size("ep")
    tokens, width = layer_input.shape
    choose = route.shape[1]
    capacity = tokens * choose * 3 // (2 * experts)
    slots = experts * capacity
    parts = (2 * capacity // 3, capacity // 3)
    gate_matrix, up_matrix, down_matrix = gate_weight[0], up_weight[0], down_weight[0]
    features, units = gate_matrix.shape
    routes, shares = route.T, gate_share.T

    me = lax.axis_index("tp")
    z, y = me // SIDE, me % SIDE
    away = np.array([0, SIDE - 1, 1, 2], np.int32)
    ahead = np.array([2, 1, 3, 0], np.int32)

    def plane(outer, inner, z_outer):
        outer, inner = np.repeat(outer, SIDE), np.tile(inner, SIDE)
        in_z, in_y = (outer, inner) if z_outer else (inner, outer)
        return ((z + in_z) % SIDE * SIDE + (y + in_y) % SIDE).astype(jnp.int32)

    gathered_order = plane(away, away, False)
    summed_order = [plane(ahead, np.arange(SIDE), True), plane(ahead, np.arange(SIDE), False)]

    sent = pl.pallas_call(
        dispatch_body,
        out_shape=jax.ShapeDtypeStruct((experts, 2 * capacity, width), BF),
        name="dispatch",
        compiler_params=vmem(16),
    )(routes, layer_input, out_grad)
    got = lax.all_to_all(sent, "ep", split_axis=0, concat_axis=0, tiled=True)
    all_g = lax.all_gather(got[:, capacity:].reshape(slots, width), "tp", axis=0, tiled=False)
    all_g = all_g.reshape(TP, experts, capacity, width)
    low = got[: experts // 2, :capacity].reshape(slots // 2, width)
    high = got[experts // 2 :, :capacity].reshape(slots // 2, width)
    pieces = plane_gather(low, z_shift, y_shift) + plane_gather(high, y_shift, z_shift)

    wide, tall = pl.pallas_call(
        turn_body,
        grid=(TP,),
        in_specs=[
            pl.BlockSpec((width, units), lambda k: (k, 0)),
            pl.BlockSpec((width, units), lambda k: (k, 0)),
            pl.BlockSpec((units, width), lambda k: (0, k)),
        ],
        out_specs=[
            pl.BlockSpec((1, 2 * units, width), lambda k: (k, 0, 0)),
            pl.BlockSpec((1, width, units), lambda k: (k, 0, 0)),
        ],
        out_shape=[
            pltpu.HBM((TP, 2 * units, width), BF),
            pltpu.HBM((TP, width, units), BF),
        ],
        name="turn",
        compiler_params=vmem(10),
    )(*in_hbm(gate_matrix, up_matrix, down_matrix))

    in_vmem = pl.BlockSpec(memory_space=pltpu.VMEM)
    in_smem = pl.BlockSpec(memory_space=pltpu.SMEM)
    stays = pl.BlockSpec(memory_space=pltpu.HBM)
    dma = pltpu.SemaphoreType.DMA
    acts = []
    per_half = len(pieces) // 2
    for first, count in ((0, SIDE - 1), (SIDE - 1, 1)):
        which = slice(0, 3) if first == 0 else slice(3, 5)
        used = pieces[:per_half][which] + pieces[per_half:][which] + acts
        shape = (2, slots // 2, 2 * units)
        last = first > 0
        acts = [
            pl.pallas_call(
                functools.partial(acts_body, first=first, count=count),
                in_specs=[in_smem] + [in_vmem] * len(used) + [stays] * 2,
                out_specs=stays if last else in_vmem,
                out_shape=pltpu.HBM(shape, F32) if last else jax.ShapeDtypeStruct(shape, F32),
                scratch_shapes=[
                    pltpu.VMEM((TP, width, 2 * units), BF),
                    pltpu.VMEM((2 * count, slots // 2, SIDE * width), BF),
                    dma((2, TP)),
                ]
                + ([pltpu.VMEM(shape, F32), dma((2,))] if last else []),
                name="acts",
                compiler_params=vmem(36),
            )(
                gathered_order,
                *used,
                *in_hbm(gate_matrix.reshape(TP, width, units), up_matrix.reshape(TP, width, units)),
            )
        ]
    acts = acts[0].reshape(experts, capacity, 2 * units)

    summed = []
    for h, part in enumerate(parts):
        rows = experts * part
        outs = pl.pallas_call(
            functools.partial(expert_body, start=sum(parts[:h])),
            in_specs=[in_smem] + [stays] * 4,
            out_specs=[in_vmem] * SIDE,
            out_shape=[jax.ShapeDtypeStruct((SIDE, rows, width), BF)] * SIDE,
            scratch_shapes=[
                pltpu.VMEM((experts, part, features), BF),
                pltpu.VMEM((TP, width, units), BF),
                pltpu.VMEM((TP, 2 * units, width), BF),
                pltpu.VMEM((experts, part, 2 * units), F32),
                pltpu.VMEM((rows, units), F32),
                pltpu.VMEM((rows, 2 * units), BF),
                dma((TP,)),
                dma((4,)),
                dma((TP,)),
                dma((1,)),
            ],
            name="expert",
            compiler_params=vmem(48),
        )(summed_order[h], *in_hbm(acts, all_g, tall, wide))
        first, second = (z_shift, y_shift) if h == 0 else (y_shift, z_shift)
        line = ring_sum(*outs, first)
        mine = ring_sum(line[2], line[1], line[3], line[0], second)
        summed.append(mine.astype(BF).reshape(experts, part, width))
    backs = [
        lax.all_to_all(jnp.concatenate(summed, axis=1), "ep", split_axis=0, concat_axis=0, tiled=True)
    ]

    return pl.pallas_call(
        combine_body,
        out_shape=jax.ShapeDtypeStruct((tokens, width), BF),
        name="combine",
        compiler_params=vmem(16),
    )(routes, shares, *backs)


def solution(mesh):
    return jax.shard_map(
        body,
        mesh=mesh,
        in_specs=(
            P("ep", "tp"),
            P("ep", "tp"),
            P("ep", None),
            P("ep", None),
            P("ep", None, "tp"),
            P("ep", None, "tp"),
            P("ep", "tp", None),
        ),
        out_specs=P("ep", "tp"),
        check_vma=False,
    )
```

```python
import functools

import jax
import jax.numpy as jnp
import numpy as np
from jax import lax
from jax.experimental import pallas as pl
from jax.experimental.pallas import tpu as pltpu
from jax.sharding import PartitionSpec as P


BF = jnp.bfloat16
F32 = jnp.float32
SIDE = 4
TP = SIDE * SIDE
ROWS_BY_ROWS = (((1,), (1,)), ((), ()))
COLS_BY_COLS = (((0,), (0,)), ((), ()))


def flat_slots(routes, experts, capacity):
    tokens = routes.shape[1]
    first, second = routes[0:1, :], routes[1:2, :]
    expert = lax.broadcasted_iota(jnp.int32, (experts, tokens), 0)
    in_first, in_second = expert == first, expert == second
    named = jnp.where(in_first | in_second, 1.0, 0.0).astype(BF)
    earlier = lax.broadcasted_iota(jnp.int32, (tokens, tokens), 0)
    later = lax.broadcasted_iota(jnp.int32, (tokens, tokens), 1)
    before = jnp.dot(named, jnp.where(earlier < later, 1.0, 0.0).astype(BF), preferred_element_type=F32)
    place_first = jnp.sum(jnp.where(in_first, before, 0.0), axis=0, keepdims=True)
    place_second = jnp.sum(jnp.where(in_second, before, 0.0), axis=0, keepdims=True)
    return (
        first * capacity + place_first.astype(jnp.int32),
        second * capacity + place_second.astype(jnp.int32),
    )


def dispatch_body(routes, inputs, grads, out):
    experts, both, _ = out.shape
    capacity = both // 2
    tokens = inputs.shape[0]
    first, second = flat_slots(routes[...], experts, capacity)
    slot = lax.broadcasted_iota(jnp.int32, (experts * capacity, tokens), 0)
    pick = jnp.where((slot == first) | (slot == second), 1.0, 0.0).astype(BF)
    for at, source in ((0, inputs), (capacity, grads)):
        rows = jnp.dot(pick, source[...], preferred_element_type=F32).astype(BF)
        for e in range(experts):
            out[e, at : at + capacity] = rows[e * capacity : (e + 1) * capacity]


def combine_body(routes, shares, *refs):
    backs, out = refs[:-1], refs[-1]
    experts, part, _ = backs[0].shape
    capacity = part * len(backs)
    tokens = out.shape[0]
    first, second = flat_slots(routes[...], experts, capacity)
    slot = lax.broadcasted_iota(jnp.int32, (experts * capacity, tokens), 0)
    share = jnp.concatenate([shares[...], jnp.zeros((6, tokens), F32)], axis=0).T
    back = jnp.concatenate([ref[e] for e in range(experts) for ref in backs], axis=0)
    one = lax.dot_general(
        jnp.where(slot == first, 1.0, 0.0).astype(BF), back, COLS_BY_COLS, preferred_element_type=F32
    )
    two = lax.dot_general(
        jnp.where(slot == second, 1.0, 0.0).astype(BF), back, COLS_BY_COLS, preferred_element_type=F32
    )
    out[...] = (one * share[:, 0:1] + two * share[:, 1:2]).astype(out.dtype)


def absorb_body(x_order, g_order, *refs, first, count, last):
    per = 3 if first == 0 else 2
    pieces, refs = (refs[:per], refs[per : 2 * per]), refs[2 * per :]
    before, refs = (refs[:2], refs[2:]) if first > 0 else ((), refs)
    gate, up, down = refs[:3]
    outs, (sides, downs, rows, sides_here, downs_here) = refs[3:-5], refs[-5:]
    width, units = gate.shape[1:]
    wide = SIDE * width

    def fetch_sides(k):
        t = x_order[first * SIDE + k]
        return [
            pltpu.make_async_copy(gate.at[t], sides.at[k, :, :units], sides_here.at[0, k]),
            pltpu.make_async_copy(up.at[t], sides.at[k, :, units:], sides_here.at[1, k]),
        ]

    def fetch_downs(i, f):
        t = g_order[(first + i) * SIDE + f]
        return pltpu.make_async_copy(
            down.at[:, pl.ds(pl.multiple_of(t * width, width), width)],
            downs.at[i, :, f * width : (f + 1) * width],
            downs_here.at[i, f],
        )

    for i in range(count):
        for f in range(SIDE):
            for copy in fetch_sides(i * SIDE + f):
                copy.start()
        for f in range(SIDE):
            fetch_downs(i, f).start()
    for kind in range(2):
        blocks = [p.at[i] for p in pieces[kind] for i in range(p.shape[0])]
        for at, block in enumerate(blocks):
            s, f = at // SIDE, at % SIDE
            rows[kind, s, :, f * width : (f + 1) * width] = block[...]

    def ring(i, carry):
        for f in range(SIDE):
            for copy in fetch_sides(i * SIDE + f):
                copy.wait()
        right = sides[pl.ds(i * SIDE, SIDE)].reshape(wide, 2 * units)
        acts_part = jnp.dot(rows[0, i], right, preferred_element_type=F32)
        for f in range(SIDE):
            fetch_downs(i, f).wait()
        hidden_part = lax.dot_general(rows[1, i], downs[i], ROWS_BY_ROWS, preferred_element_type=F32)
        if last:
            form_grads(before[0][...] + acts_part, before[1][...] + hidden_part, *outs)
        else:

            @pl.when(i == 0)
            def _():
                outs[0][...] = acts_part
                outs[1][...] = hidden_part

            @pl.when(i != 0)
            def _():
                outs[0][...] += acts_part
                outs[1][...] += hidden_part

        return carry

    lax.fori_loop(0, count, ring, 0)


def form_grads(acts, hidden, *outs):
    units = hidden.shape[1]
    gate, up = acts[:, :units], acts[:, units:]
    sigma = jax.nn.sigmoid(gate)
    slope = sigma * (1.0 + gate * (1.0 - sigma))
    for_gate = (hidden * up * slope).astype(BF)
    for_up = (hidden * gate * sigma).astype(BF)
    experts = outs[0].shape[0]
    start = 0
    for out in outs:
        part = out.shape[1]
        for b in range(experts):
            here = slice(b * hidden.shape[0] // experts + start, b * hidden.shape[0] // experts + start + part)
            out[b, :, :units] = for_gate[here]
            out[b, :, units:] = for_up[here]
        start += part


def parts_body(order, grads, gate, up, *refs):
    outs, (sides, sides_here) = refs[:SIDE], refs[SIDE:]
    experts, part_rows, _ = grads.shape
    width, units = gate.shape[1:]

    def fetch(k):
        return [
            pltpu.make_async_copy(gate.at[order[k]], sides.at[k, :, :units], sides_here.at[0, k]),
            pltpu.make_async_copy(up.at[order[k]], sides.at[k, :, units:], sides_here.at[1, k]),
        ]

    for k in range(TP):
        for copy in fetch(k):
            copy.start()

    def members(j, carry):
        k = 2 * j
        for copy in fetch(k) + fetch(k + 1):
            copy.wait()
        part = lax.dot_general(
            grads[...].reshape(experts * part_rows, 2 * units),
            sides[pl.ds(k, 2)].reshape(2 * width, 2 * units),
            ROWS_BY_ROWS,
            preferred_element_type=F32,
        ).astype(BF)
        for f in range(SIDE):

            @pl.when(k // SIDE == f)
            def _():
                outs[f][k % SIDE] = part[:, :width]
                outs[f][k % SIDE + 1] = part[:, width:]

        return carry

    lax.fori_loop(0, TP // 2, members, 0)


def vmem(mebibytes):
    return pltpu.CompilerParams(vmem_limit_bytes=mebibytes << 20)


def in_hbm(*arrays):
    return [pltpu.with_memory_space_constraint(a, pltpu.HBM) for a in arrays]


def z_shift(by):
    return [(z * SIDE + y, (z + by) % SIDE * SIDE + y) for z in range(SIDE) for y in range(SIDE)]


def y_shift(by):
    return [(z * SIDE + y, z * SIDE + (y + by) % SIDE) for z in range(SIDE) for y in range(SIDE)]


def shifted(x, shift, by):
    return lax.ppermute(x, "tp", shift(by))


def ring_gather(x, shift):
    half = x.shape[0] // 2
    below = shifted(x, shift, 1)
    above = shifted(x, shift, 3)
    far_low = shifted(below[:half], shift, 1)
    far_high = shifted(above[half:], shift, 3)
    return [x, below, above, far_low, far_high]


def plane_gather(x, first, second):
    rows, width = x.shape
    line = jnp.concatenate(ring_gather(x, first), axis=0)
    return [piece.reshape(-1, rows, width) for piece in ring_gather(line, second)]


def ring_sum(far, ahead, behind, own, shift):
    total = own.astype(F32)
    for by, part in ((2, far), (1, ahead), (3, behind)):
        total = total + shifted(part.astype(BF), shift, by).astype(F32)
    return total


def body(layer_input, out_grad, route, gate_share, gate_weight, up_weight, down_weight):
    experts = lax.axis_size("ep")
    tokens, width = layer_input.shape
    choose = route.shape[1]
    capacity = tokens * choose * 3 // (2 * experts)
    slots = experts * capacity
    parts = (2 * capacity // 3, capacity // 3)
    gate_matrix, up_matrix, down_matrix = gate_weight[0], up_weight[0], down_weight[0]
    _, units = gate_matrix.shape
    routes, shares = route.T, gate_share.T

    me = lax.axis_index("tp")
    z, y = me // SIDE, me % SIDE
    away = np.array([0, SIDE - 1, 1, 2], np.int32)
    ahead = np.array([2, 1, 3, 0], np.int32)

    def plane(outer, inner, z_outer):
        outer, inner = np.repeat(outer, SIDE), np.tile(inner, SIDE)
        in_z, in_y = (outer, inner) if z_outer else (inner, outer)
        return ((z + in_z) % SIDE * SIDE + (y + in_y) % SIDE).astype(jnp.int32)

    x_order, g_order = plane(away, away, False), plane(away, away, True)
    summed_order = [plane(ahead, np.arange(SIDE), True), plane(ahead, np.arange(SIDE), False)]

    sent = pl.pallas_call(
        dispatch_body,
        out_shape=jax.ShapeDtypeStruct((experts, 2 * capacity, width), BF),
        name="dispatch",
        compiler_params=vmem(16),
    )(routes, layer_input, out_grad)
    got = lax.all_to_all(sent, "ep", split_axis=0, concat_axis=0, tiled=True)
    x = plane_gather(got[:, :capacity].reshape(slots, width), z_shift, y_shift)
    g = plane_gather(got[:, capacity:].reshape(slots, width), y_shift, z_shift)

    in_vmem = pl.BlockSpec(memory_space=pltpu.VMEM)
    in_smem = pl.BlockSpec(memory_space=pltpu.SMEM)
    stays = pl.BlockSpec(memory_space=pltpu.HBM)
    dma = pltpu.SemaphoreType.DMA
    sums = []
    for first, count in ((0, SIDE - 1), (SIDE - 1, 1)):
        last = first > 0
        which = slice(3, 5) if last else slice(0, 3)
        if last:
            outs = [jax.ShapeDtypeStruct((experts, part, 2 * units), BF) for part in parts]
        else:
            outs = [jax.ShapeDtypeStruct((slots, 2 * units), F32), jax.ShapeDtypeStruct((slots, units), F32)]
        used = [*x[which], *g[which], *sums]
        sums = pl.pallas_call(
            functools.partial(absorb_body, first=first, count=count, last=last),
            in_specs=[in_smem] * 2 + [in_vmem] * len(used) + [stays] * 3,
            out_specs=[in_vmem] * 2,
            out_shape=outs,
            scratch_shapes=[
                pltpu.VMEM((count * SIDE, width, 2 * units), BF),
                pltpu.VMEM((count, units, SIDE * width), BF),
                pltpu.VMEM((2, count, slots, SIDE * width), BF),
                dma((2, count * SIDE)),
                dma((count, SIDE)),
            ],
            name="absorb",
            compiler_params=vmem(44),
        )(
            x_order,
            g_order,
            *used,
            *in_hbm(
                gate_matrix.reshape(TP, width, units), up_matrix.reshape(TP, width, units), down_matrix
            ),
        )

    summed = []
    for h, part in enumerate(parts):
        rows = experts * part
        outs = pl.pallas_call(
            parts_body,
            in_specs=[in_smem, in_vmem] + [stays] * 2,
            out_specs=[in_vmem] * SIDE,
            out_shape=[jax.ShapeDtypeStruct((SIDE, rows, width), BF)] * SIDE,
            scratch_shapes=[pltpu.VMEM((TP, width, 2 * units), BF), dma((2, TP))],
            name="parts",
            compiler_params=vmem(32),
        )(summed_order[h], sums[h], *in_hbm(gate_matrix.reshape(TP, width, units), up_matrix.reshape(TP, width, units)))
        first, second = (z_shift, y_shift) if h == 0 else (y_shift, z_shift)
        line = ring_sum(*outs, first)
        mine = ring_sum(line[2], line[1], line[3], line[0], second)
        summed.append(mine.astype(BF).reshape(experts, part, width))
    backs = [
        lax.all_to_all(jnp.concatenate(summed, axis=1), "ep", split_axis=0, concat_axis=0, tiled=True)
    ]

    return pl.pallas_call(
        combine_body,
        out_shape=jax.ShapeDtypeStruct((tokens, width), BF),
        name="combine",
        compiler_params=vmem(16),
    )(routes, shares, *backs)


def solution(mesh):
    return jax.shard_map(
        body,
        mesh=mesh,
        in_specs=(
            P("ep", "tp"),
            P("ep", "tp"),
            P("ep", None),
            P("ep", None),
            P("ep", None, "tp"),
            P("ep", None, "tp"),
            P("ep", "tp", None),
        ),
        out_specs=P("ep", "tp"),
        check_vma=False,
    )
```

```python
import functools

import jax
import jax.numpy as jnp
import numpy as np
from jax import lax
from jax.experimental import pallas as pl
from jax.experimental.pallas import tpu as pltpu
from jax.sharding import PartitionSpec as P


BF = jnp.bfloat16
F32 = jnp.float32
SIDE = 4
TP = SIDE * SIDE
ROWS_BY_ROWS = (((1,), (1,)), ((), ()))
COLS_BY_COLS = (((0,), (0,)), ((), ()))


def flat_slots(routes, experts, capacity):
    tokens = routes.shape[1]
    first, second = routes[0:1, :], routes[1:2, :]
    expert = lax.broadcasted_iota(jnp.int32, (experts, tokens), 0)
    in_first, in_second = expert == first, expert == second
    named = jnp.where(in_first | in_second, 1.0, 0.0).astype(BF)
    earlier = lax.broadcasted_iota(jnp.int32, (tokens, tokens), 0)
    later = lax.broadcasted_iota(jnp.int32, (tokens, tokens), 1)
    before = jnp.dot(named, jnp.where(earlier < later, 1.0, 0.0).astype(BF), preferred_element_type=F32)
    place_first = jnp.sum(jnp.where(in_first, before, 0.0), axis=0, keepdims=True)
    place_second = jnp.sum(jnp.where(in_second, before, 0.0), axis=0, keepdims=True)
    return (
        first * capacity + place_first.astype(jnp.int32),
        second * capacity + place_second.astype(jnp.int32),
    )


def dispatch_body(routes, inputs, grads, out):
    experts, both, _ = out.shape
    capacity = both // 2
    tokens = inputs.shape[0]
    first, second = flat_slots(routes[...], experts, capacity)
    slot = lax.broadcasted_iota(jnp.int32, (experts * capacity, tokens), 0)
    pick = jnp.where((slot == first) | (slot == second), 1.0, 0.0).astype(BF)
    for at, source in ((0, inputs), (capacity, grads)):
        rows = jnp.dot(pick, source[...], preferred_element_type=F32).astype(BF)
        for e in range(experts):
            out[e, at : at + capacity] = rows[e * capacity : (e + 1) * capacity]


def combine_body(routes, shares, *refs):
    backs, out = refs[:-1], refs[-1]
    experts, part, _ = backs[0].shape
    capacity = part * len(backs)
    tokens = out.shape[0]
    first, second = flat_slots(routes[...], experts, capacity)
    slot = lax.broadcasted_iota(jnp.int32, (experts * capacity, tokens), 0)
    share = jnp.concatenate([shares[...], jnp.zeros((6, tokens), F32)], axis=0).T
    back = jnp.concatenate([ref[e] for e in range(experts) for ref in backs], axis=0)
    one = lax.dot_general(
        jnp.where(slot == first, 1.0, 0.0).astype(BF), back, COLS_BY_COLS, preferred_element_type=F32
    )
    two = lax.dot_general(
        jnp.where(slot == second, 1.0, 0.0).astype(BF), back, COLS_BY_COLS, preferred_element_type=F32
    )
    out[...] = (one * share[:, 0:1] + two * share[:, 1:2]).astype(out.dtype)


def absorb_body(x_order, g_order, *refs, first, count, last):
    per = 2 if last else count
    pieces, refs = (refs[:per], refs[per : 2 * per]), refs[2 * per :]
    before, refs = (refs[:2], refs[2:]) if first > 0 else ((), refs)
    gate, up, down = refs[:3]
    outs, (sides, downs, sides_here, downs_here), rows = refs[3:5], refs[5:9], refs[9:]
    width, units = gate.shape[1:]
    wide = SIDE * width

    def fetch_sides(k):
        t = x_order[first * SIDE + k]
        return [
            pltpu.make_async_copy(gate.at[t], sides.at[k, :, :units], sides_here.at[0, k]),
            pltpu.make_async_copy(up.at[t], sides.at[k, :, units:], sides_here.at[1, k]),
        ]

    def fetch_downs(i, f):
        t = g_order[(first + i) * SIDE + f]
        return pltpu.make_async_copy(
            down.at[:, pl.ds(pl.multiple_of(t * width, width), width)],
            downs.at[i, :, f * width : (f + 1) * width],
            downs_here.at[i, f],
        )

    for i in range(count):
        for f in range(SIDE):
            for copy in fetch_sides(i * SIDE + f):
                copy.start()
        for f in range(SIDE):
            fetch_downs(i, f).start()
    blocks = [[p.at[i] for p in pieces[kind] for i in range(p.shape[0])] for kind in range(2)]
    if count > 1:
        for kind in range(2):
            for at, block in enumerate(blocks[kind]):
                s, f = at // SIDE, at % SIDE
                rows[0][kind, s, :, f * width : (f + 1) * width] = block[...]

    def left(kind, i):
        if count > 1:
            return rows[0][kind, i]
        return jnp.concatenate([block[...] for block in blocks[kind]], axis=1)

    def ring(i, carry):
        for f in range(SIDE):
            for copy in fetch_sides(i * SIDE + f):
                copy.wait()
        right = sides[pl.ds(i * SIDE, SIDE)].reshape(wide, 2 * units)
        acts_part = jnp.dot(left(0, i), right, preferred_element_type=F32)
        for f in range(SIDE):
            fetch_downs(i, f).wait()
        hidden_part = lax.dot_general(left(1, i), downs[i], ROWS_BY_ROWS, preferred_element_type=F32)
        if last:
            form_grads(before[0][...] + acts_part, before[1][...] + hidden_part, *outs)
        elif count == 1:
            outs[0][...] = acts_part
            outs[1][...] = hidden_part
        else:

            @pl.when(i == 0)
            def _():
                outs[0][...] = before[0][...] + acts_part
                outs[1][...] = before[1][...] + hidden_part

            @pl.when(i != 0)
            def _():
                outs[0][...] += acts_part
                outs[1][...] += hidden_part

        return carry

    if count > 1:
        lax.fori_loop(0, count, ring, 0)
    else:
        ring(0, 0)


def form_grads(acts, hidden, *outs):
    units = hidden.shape[1]
    gate, up = acts[:, :units], acts[:, units:]
    sigma = jax.nn.sigmoid(gate)
    slope = sigma * (1.0 + gate * (1.0 - sigma))
    for_gate = hidden * up * slope
    for_up = hidden * gate * sigma
    experts = outs[0].shape[0]
    start = 0
    for out in outs:
        part = out.shape[1]
        for b in range(experts):
            here = slice(b * hidden.shape[0] // experts + start, b * hidden.shape[0] // experts + start + part)
            out[b, :, :units] = for_gate[here].astype(BF)
            out[b, :, units:] = for_up[here].astype(BF)
        start += part


def parts_body(order, grads, gate, up, *refs):
    outs, (sides, sides_here) = refs[:SIDE], refs[SIDE:]
    experts, part_rows, _ = grads.shape
    width, units = gate.shape[1:]

    def fetch(k):
        return [
            pltpu.make_async_copy(gate.at[order[k]], sides.at[k, :, :units], sides_here.at[0, k]),
            pltpu.make_async_copy(up.at[order[k]], sides.at[k, :, units:], sides_here.at[1, k]),
        ]

    for k in range(TP):
        for copy in fetch(k):
            copy.start()

    def members(j, carry):
        k = 2 * j
        for copy in fetch(k) + fetch(k + 1):
            copy.wait()
        part = lax.dot_general(
            grads[...].reshape(experts * part_rows, 2 * units),
            sides[pl.ds(k, 2)].reshape(2 * width, 2 * units),
            ROWS_BY_ROWS,
            preferred_element_type=F32,
        ).astype(BF)
        for f in range(SIDE):

            @pl.when(k // SIDE == f)
            def _():
                outs[f][k % SIDE] = part[:, :width]
                outs[f][k % SIDE + 1] = part[:, width:]

        return carry

    lax.fori_loop(0, TP // 2, members, 0)


def vmem(mebibytes):
    return pltpu.CompilerParams(vmem_limit_bytes=mebibytes << 20)


def in_hbm(*arrays):
    return [pltpu.with_memory_space_constraint(a, pltpu.HBM) for a in arrays]


def z_shift(by):
    return [(z * SIDE + y, (z + by) % SIDE * SIDE + y) for z in range(SIDE) for y in range(SIDE)]


def y_shift(by):
    return [(z * SIDE + y, z * SIDE + (y + by) % SIDE) for z in range(SIDE) for y in range(SIDE)]


def shifted(x, shift, by):
    return lax.ppermute(x, "tp", shift(by))


def ring_gather(x, shift):
    half = x.shape[0] // 2
    below = shifted(x, shift, 1)
    above = shifted(x, shift, 3)
    far_low = shifted(below[:half], shift, 1)
    far_high = shifted(above[half:], shift, 3)
    return [x, below, above, far_low, far_high]


def plane_gather(x, first, second):
    rows, width = x.shape
    line = jnp.concatenate(ring_gather(x, first), axis=0)
    return [piece.reshape(-1, rows, width) for piece in ring_gather(line, second)]


def ring_sum(far, ahead, behind, own, shift):
    total = own.astype(F32)
    for by, part in ((2, far), (1, ahead), (3, behind)):
        total = total + shifted(part.astype(BF), shift, by).astype(F32)
    return total


def body(layer_input, out_grad, route, gate_share, gate_weight, up_weight, down_weight):
    experts = lax.axis_size("ep")
    tokens, width = layer_input.shape
    choose = route.shape[1]
    capacity = tokens * choose * 3 // (2 * experts)
    slots = experts * capacity
    parts = (7 * capacity // 12, 5 * capacity // 12)
    gate_matrix, up_matrix, down_matrix = gate_weight[0], up_weight[0], down_weight[0]
    _, units = gate_matrix.shape
    routes, shares = route.T, gate_share.T

    me = lax.axis_index("tp")
    z, y = me // SIDE, me % SIDE
    away = np.array([0, SIDE - 1, 1, 2], np.int32)
    ahead = np.array([2, 1, 3, 0], np.int32)

    def plane(outer, inner, z_outer):
        outer, inner = np.repeat(outer, SIDE), np.tile(inner, SIDE)
        in_z, in_y = (outer, inner) if z_outer else (inner, outer)
        return ((z + in_z) % SIDE * SIDE + (y + in_y) % SIDE).astype(jnp.int32)

    x_order, g_order = plane(away, away, False), plane(away, away, True)
    summed_order = [plane(ahead, np.arange(SIDE), True), plane(ahead, np.arange(SIDE), False)]

    sent = pl.pallas_call(
        dispatch_body,
        out_shape=jax.ShapeDtypeStruct((experts, 2 * capacity, width), BF),
        name="dispatch",
        compiler_params=vmem(16),
    )(routes, layer_input, out_grad)
    got = lax.all_to_all(sent, "ep", split_axis=0, concat_axis=0, tiled=True)
    x = plane_gather(got[:, :capacity].reshape(slots, width), z_shift, y_shift)
    g = plane_gather(got[:, capacity:].reshape(slots, width), y_shift, z_shift)

    in_vmem = pl.BlockSpec(memory_space=pltpu.VMEM)
    in_smem = pl.BlockSpec(memory_space=pltpu.SMEM)
    stays = pl.BlockSpec(memory_space=pltpu.HBM)
    dma = pltpu.SemaphoreType.DMA
    sums = []
    for first, count, which, limit in ((0, 1, slice(0, 1), 28), (1, 2, slice(1, 3), 34), (3, 1, slice(3, 5), 28)):
        last = first + count == SIDE
        if last:
            outs = [jax.ShapeDtypeStruct((experts, part, 2 * units), BF) for part in parts]
        else:
            outs = [jax.ShapeDtypeStruct((slots, 2 * units), F32), jax.ShapeDtypeStruct((slots, units), F32)]
        used = [*x[which], *g[which], *sums]
        sums = pl.pallas_call(
            functools.partial(absorb_body, first=first, count=count, last=last),
            in_specs=[in_smem] * 2 + [in_vmem] * len(used) + [stays] * 3,
            out_specs=[in_vmem] * 2,
            out_shape=outs,
            scratch_shapes=[
                pltpu.VMEM((count * SIDE, width, 2 * units), BF),
                pltpu.VMEM((count, units, SIDE * width), BF),
                dma((2, count * SIDE)),
                dma((count, SIDE)),
            ]
            + [pltpu.VMEM((2, count, slots, SIDE * width), BF)] * (count > 1),
            name="absorb",
            compiler_params=vmem(limit),
        )(
            x_order,
            g_order,
            *used,
            *in_hbm(
                gate_matrix.reshape(TP, width, units), up_matrix.reshape(TP, width, units), down_matrix
            ),
        )

    summed = []
    for h, part in enumerate(parts):
        rows = experts * part
        outs = pl.pallas_call(
            parts_body,
            in_specs=[in_smem, in_vmem] + [stays] * 2,
            out_specs=[in_vmem] * SIDE,
            out_shape=[jax.ShapeDtypeStruct((SIDE, rows, width), BF)] * SIDE,
            scratch_shapes=[pltpu.VMEM((TP, width, 2 * units), BF), dma((2, TP))],
            name="parts",
            compiler_params=vmem(32),
        )(summed_order[h], sums[h], *in_hbm(gate_matrix.reshape(TP, width, units), up_matrix.reshape(TP, width, units)))
        first, second = (z_shift, y_shift) if h == 0 else (y_shift, z_shift)
        line = ring_sum(*outs, first)
        mine = ring_sum(line[2], line[1], line[3], line[0], second)
        summed.append(mine.astype(BF).reshape(experts, part, width))
    backs = [
        lax.all_to_all(jnp.concatenate(summed, axis=1), "ep", split_axis=0, concat_axis=0, tiled=True)
    ]

    return pl.pallas_call(
        combine_body,
        out_shape=jax.ShapeDtypeStruct((tokens, width), BF),
        name="combine",
        compiler_params=vmem(16),
    )(routes, shares, *backs)


def solution(mesh):
    return jax.shard_map(
        body,
        mesh=mesh,
        in_specs=(
            P("ep", "tp"),
            P("ep", "tp"),
            P("ep", None),
            P("ep", None),
            P("ep", None, "tp"),
            P("ep", None, "tp"),
            P("ep", "tp", None),
        ),
        out_specs=P("ep", "tp"),
        check_vma=False,
    )
```

```python
import functools

import jax
import jax.numpy as jnp
import numpy as np
from jax import lax
from jax.experimental import pallas as pl
from jax.experimental.pallas import tpu as pltpu
from jax.sharding import PartitionSpec as P


BF = jnp.bfloat16
F32 = jnp.float32
SIDE = 4
TP = SIDE * SIDE
ROWS_BY_ROWS = (((1,), (1,)), ((), ()))
COLS_BY_COLS = (((0,), (0,)), ((), ()))


def flat_slots(routes, experts, capacity):
    tokens = routes.shape[1]
    first, second = routes[0:1, :], routes[1:2, :]
    expert = lax.broadcasted_iota(jnp.int32, (experts, tokens), 0)
    in_first, in_second = expert == first, expert == second
    named = jnp.where(in_first | in_second, 1.0, 0.0).astype(BF)
    earlier = lax.broadcasted_iota(jnp.int32, (tokens, tokens), 0)
    later = lax.broadcasted_iota(jnp.int32, (tokens, tokens), 1)
    before = jnp.dot(named, jnp.where(earlier < later, 1.0, 0.0).astype(BF), preferred_element_type=F32)
    place_first = jnp.sum(jnp.where(in_first, before, 0.0), axis=0, keepdims=True)
    place_second = jnp.sum(jnp.where(in_second, before, 0.0), axis=0, keepdims=True)
    return (
        first * capacity + place_first.astype(jnp.int32),
        second * capacity + place_second.astype(jnp.int32),
    )


def dispatch_body(routes, inputs, grads, out):
    experts, both, _ = out.shape
    capacity = both // 2
    tokens = inputs.shape[0]
    first, second = flat_slots(routes[...], experts, capacity)
    slot = lax.broadcasted_iota(jnp.int32, (experts * capacity, tokens), 0)
    pick = jnp.where((slot == first) | (slot == second), 1.0, 0.0).astype(BF)
    for at, source in ((0, inputs), (capacity, grads)):
        rows = jnp.dot(pick, source[...], preferred_element_type=F32).astype(BF)
        for e in range(experts):
            out[e, at : at + capacity] = rows[e * capacity : (e + 1) * capacity]


def combine_body(routes, shares, *refs):
    backs, out = refs[:-1], refs[-1]
    experts, part, _ = backs[0].shape
    capacity = part * len(backs)
    tokens = out.shape[0]
    first, second = flat_slots(routes[...], experts, capacity)
    slot = lax.broadcasted_iota(jnp.int32, (experts * capacity, tokens), 0)
    share = jnp.concatenate([shares[...], jnp.zeros((6, tokens), F32)], axis=0).T
    back = jnp.concatenate([ref[e] for e in range(experts) for ref in backs], axis=0)
    one = lax.dot_general(
        jnp.where(slot == first, 1.0, 0.0).astype(BF), back, COLS_BY_COLS, preferred_element_type=F32
    )
    two = lax.dot_general(
        jnp.where(slot == second, 1.0, 0.0).astype(BF), back, COLS_BY_COLS, preferred_element_type=F32
    )
    out[...] = (one * share[:, 0:1] + two * share[:, 1:2]).astype(out.dtype)


def weight_copies(x_order, g_order, hbm, vmem, here, first, count):
    (gate, up, down), (sides, downs), (sides_here, downs_here) = hbm, vmem, here
    width, units = gate.shape[1:]

    def for_acts(k):
        t = x_order[first * SIDE + k]
        return [
            pltpu.make_async_copy(gate.at[t], sides.at[k, :, :units], sides_here.at[0, k]),
            pltpu.make_async_copy(up.at[t], sides.at[k, :, units:], sides_here.at[1, k]),
        ]

    def for_hidden(i, f):
        t = g_order[(first + i) * SIDE + f]
        return pltpu.make_async_copy(
            down.at[:, pl.ds(pl.multiple_of(t * width, width), width)],
            downs.at[i, :, f * width : (f + 1) * width],
            downs_here.at[i, f],
        )

    def every():
        for i in range(count):
            for f in range(SIDE):
                yield from for_acts(i * SIDE + f)
            for f in range(SIDE):
                yield for_hidden(i, f)

    return for_acts, for_hidden, every


def absorb_body(x_order, g_order, *refs, first, count, ahead):
    pieces, refs = (refs[:count], refs[count : 2 * count]), refs[2 * count :]
    given = first > 0
    before, refs = (refs[:4], refs[4:]) if given else ((), refs)
    hbm, outs, refs = refs[:3], refs[3:7], refs[7:]
    following = weight_copies(x_order, g_order, hbm, outs[2:], refs[:2], first + count, ahead)[2]
    if given:
        sides, downs = before[2:]
    else:
        sides, downs = refs[2:4]
        for_acts, for_hidden, every = weight_copies(x_order, g_order, hbm, refs[2:4], refs[4:6], first, count)
        for copy in every():
            copy.start()
    for copy in following():
        copy.start()
    wide = SIDE * hbm[0].shape[1]
    left = [jnp.concatenate([pieces[kind][0][f] for f in range(SIDE)], axis=1) for kind in range(2)]
    if not given:
        for f in range(SIDE):
            for copy in for_acts(f):
                copy.wait()
    part = jnp.dot(left[0], sides[...].reshape(wide, sides.shape[2]), preferred_element_type=F32)
    outs[0][...] = before[0][...] + part if given else part
    if not given:
        for f in range(SIDE):
            for_hidden(0, f).wait()
    part = lax.dot_general(left[1], downs[0], ROWS_BY_ROWS, preferred_element_type=F32)
    outs[1][...] = before[1][...] + part if given else part
    for copy in following():
        copy.wait()


def finish_body(order, *refs):
    pieces, (acts, hidden, sides, downs, gate, up) = (refs[:2], refs[2:4]), refs[4:10]
    outs, later, (grads, wide, wide_here) = refs[10 : 10 + SIDE], refs[10 + SIDE], refs[11 + SIDE :]
    start_parts(order, gate, up, wide, wide_here)
    left = [jnp.concatenate([p[i] for p in pieces[kind] for i in range(p.shape[0])], axis=1) for kind in range(2)]
    right = sides[...].reshape(left[0].shape[1], sides.shape[2])
    form_grads(
        acts[...] + jnp.dot(left[0], right, preferred_element_type=F32),
        hidden[...] + lax.dot_general(left[1], downs[0], ROWS_BY_ROWS, preferred_element_type=F32),
        grads,
        later,
    )
    form_parts(order, grads, gate, up, wide, wide_here, outs)


def form_grads(acts, hidden, *outs):
    units = hidden.shape[1]
    gate, up = acts[:, :units], acts[:, units:]
    sigma = jax.nn.sigmoid(gate)
    slope = sigma * (1.0 + gate * (1.0 - sigma))
    for_gate = hidden * up * slope
    for_up = hidden * gate * sigma
    experts = outs[0].shape[0]
    start = 0
    for out in outs:
        part = out.shape[1]
        for b in range(experts):
            here = slice(b * hidden.shape[0] // experts + start, b * hidden.shape[0] // experts + start + part)
            out[b, :, :units] = for_gate[here].astype(BF)
            out[b, :, units:] = for_up[here].astype(BF)
        start += part


def part_copies(order, gate, up, sides, here, k):
    units = gate.shape[2]
    return [
        pltpu.make_async_copy(gate.at[order[k]], sides.at[k, :, :units], here.at[0, k]),
        pltpu.make_async_copy(up.at[order[k]], sides.at[k, :, units:], here.at[1, k]),
    ]


def start_parts(order, gate, up, sides, here):
    for k in range(TP):
        for copy in part_copies(order, gate, up, sides, here, k):
            copy.start()


def form_parts(order, grads, gate, up, sides, here, outs):
    experts, part_rows, both = grads.shape
    width = gate.shape[1]

    def members(j, carry):
        k = 2 * j
        for copy in part_copies(order, gate, up, sides, here, k) + part_copies(order, gate, up, sides, here, k + 1):
            copy.wait()
        part = lax.dot_general(
            grads[...].reshape(experts * part_rows, both),
            sides[pl.ds(k, 2)].reshape(2 * width, both),
            ROWS_BY_ROWS,
            preferred_element_type=F32,
        ).astype(BF)
        for f in range(SIDE):

            @pl.when(k // SIDE == f)
            def _():
                outs[f][k % SIDE] = part[:, :width]
                outs[f][k % SIDE + 1] = part[:, width:]

        return carry

    lax.fori_loop(0, TP // 2, members, 0)


def parts_body(order, grads, gate, up, *refs):
    outs, (sides, here) = refs[:SIDE], refs[SIDE:]
    start_parts(order, gate, up, sides, here)
    form_parts(order, grads, gate, up, sides, here, outs)


def vmem(mebibytes):
    return pltpu.CompilerParams(vmem_limit_bytes=mebibytes << 20)


def in_hbm(*arrays):
    return [pltpu.with_memory_space_constraint(a, pltpu.HBM) for a in arrays]


def z_shift(by):
    return [(z * SIDE + y, (z + by) % SIDE * SIDE + y) for z in range(SIDE) for y in range(SIDE)]


def y_shift(by):
    return [(z * SIDE + y, z * SIDE + (y + by) % SIDE) for z in range(SIDE) for y in range(SIDE)]


def shifted(x, shift, by):
    return lax.ppermute(x, "tp", shift(by))


def ring_gather(x, shift):
    half = x.shape[0] // 2
    below = shifted(x, shift, 1)
    above = shifted(x, shift, 3)
    far_low = shifted(below[:half], shift, 1)
    far_high = shifted(above[half:], shift, 3)
    return [x, below, above, far_low, far_high]


def plane_gather(x, first, second):
    rows, width = x.shape
    far, below, above = [shifted(x, first, by) for by in (2, 1, 3)]
    line = jnp.concatenate([x, below, above, far], axis=0)
    return [piece.reshape(-1, rows, width) for piece in ring_gather(line, second)]


def ring_sum(far, ahead, behind, own, shift):
    total = own.astype(F32)
    for by, part in ((2, far), (1, ahead), (3, behind)):
        total = total + shifted(part.astype(BF), shift, by).astype(F32)
    return total


def body(layer_input, out_grad, route, gate_share, gate_weight, up_weight, down_weight):
    experts = lax.axis_size("ep")
    tokens, width = layer_input.shape
    choose = route.shape[1]
    capacity = tokens * choose * 3 // (2 * experts)
    slots = experts * capacity
    parts = (7 * capacity // 12, 5 * capacity // 12)
    gate_matrix, up_matrix, down_matrix = gate_weight[0], up_weight[0], down_weight[0]
    _, units = gate_matrix.shape
    routes, shares = route.T, gate_share.T

    me = lax.axis_index("tp")
    z, y = me // SIDE, me % SIDE
    away = np.array([0, SIDE - 1, 1, 2], np.int32)
    ahead = np.array([2, 1, 3, 0], np.int32)

    def plane(outer, inner, z_outer):
        outer, inner = np.repeat(outer, SIDE), np.tile(inner, SIDE)
        in_z, in_y = (outer, inner) if z_outer else (inner, outer)
        return ((z + in_z) % SIDE * SIDE + (y + in_y) % SIDE).astype(jnp.int32)

    x_order, g_order = plane(away, away, False), plane(away, away, True)
    summed_order = [plane(ahead, np.arange(SIDE), True), plane(ahead, np.arange(SIDE), False)]

    sent = pl.pallas_call(
        dispatch_body,
        out_shape=jax.ShapeDtypeStruct((experts, 2 * capacity, width), BF),
        name="dispatch",
        compiler_params=vmem(16),
    )(routes, *in_hbm(layer_input, out_grad))
    got = lax.all_to_all(sent, "ep", split_axis=0, concat_axis=0, tiled=True)
    x = plane_gather(got[:, :capacity].reshape(slots, width), z_shift, y_shift)
    g = plane_gather(got[:, capacity:].reshape(slots, width), y_shift, z_shift)

    in_vmem = pl.BlockSpec(memory_space=pltpu.VMEM)
    in_smem = pl.BlockSpec(memory_space=pltpu.SMEM)
    stays = pl.BlockSpec(memory_space=pltpu.HBM)
    dma = pltpu.SemaphoreType.DMA
    sides_of = lambda count: pltpu.VMEM((count * SIDE, width, 2 * units), BF)
    downs_of = lambda count: pltpu.VMEM((count, units, SIDE * width), BF)
    blocks = in_hbm(gate_matrix.reshape(TP, width, units), up_matrix.reshape(TP, width, units), down_matrix)
    state = []
    for first, count, ahead, limit in ((0, 1, 1, 14), (1, 1, 1, 18), (2, 1, 1, 18)):
        used = [*x[first : first + count], *g[first : first + count], *state]
        own = []
        if first == 0:
            own = [sides_of(count), downs_of(count), dma((2, count * SIDE)), dma((count, SIDE))]
        state = pl.pallas_call(
            functools.partial(absorb_body, first=first, count=count, ahead=ahead),
            in_specs=[in_smem] * 2 + [in_vmem] * len(used) + [stays] * 3,
            out_specs=[in_vmem] * 4,
            out_shape=[
                jax.ShapeDtypeStruct((slots, 2 * units), F32),
                jax.ShapeDtypeStruct((slots, units), F32),
                jax.ShapeDtypeStruct((ahead * SIDE, width, 2 * units), BF),
                jax.ShapeDtypeStruct((ahead, units, SIDE * width), BF),
            ],
            scratch_shapes=[dma((2, ahead * SIDE)), dma((ahead, SIDE))] + own,
            name="absorb",
            compiler_params=vmem(limit),
        )(x_order, g_order, *used, *blocks)

    def parts_shape(part):
        return [jax.ShapeDtypeStruct((SIDE, experts * part, width), BF)] * SIDE

    summed = []
    for h, part in enumerate(parts):
        if h == 0:
            later_shape = jax.ShapeDtypeStruct((experts, parts[1], 2 * units), BF)
            *outs, later = pl.pallas_call(
                finish_body,
                in_specs=[in_smem] + [in_vmem] * 8 + [stays] * 2,
                out_specs=[in_vmem] * (SIDE + 1),
                out_shape=parts_shape(part) + [later_shape],
                scratch_shapes=[pltpu.VMEM((experts, part, 2 * units), BF), sides_of(SIDE), dma((2, TP))],
                name="finish",
                compiler_params=vmem(29),
            )(summed_order[h], *x[3:], *g[3:], *state, *blocks[:2])
        else:
            outs = pl.pallas_call(
                parts_body,
                in_specs=[in_smem, in_vmem] + [stays] * 2,
                out_specs=[in_vmem] * SIDE,
                out_shape=parts_shape(part),
                scratch_shapes=[sides_of(SIDE), dma((2, TP))],
                name="parts",
                compiler_params=vmem(28),
            )(summed_order[h], later, *blocks[:2])
        first, second = (z_shift, y_shift) if h == 0 else (y_shift, z_shift)
        line = ring_sum(*outs, first)
        mine = ring_sum(line[2], line[1], line[3], line[0], second)
        summed.append(mine.astype(BF).reshape(experts, part, width))
    backs = [
        lax.all_to_all(jnp.concatenate(summed, axis=1), "ep", split_axis=0, concat_axis=0, tiled=True)
    ]

    return pl.pallas_call(
        combine_body,
        out_shape=jax.ShapeDtypeStruct((tokens, width), BF),
        name="combine",
        compiler_params=vmem(16),
    )(routes, shares, *backs)


def solution(mesh):
    return jax.shard_map(
        body,
        mesh=mesh,
        in_specs=(
            P("ep", "tp"),
            P("ep", "tp"),
            P("ep", None),
            P("ep", None),
            P("ep", None, "tp"),
            P("ep", None, "tp"),
            P("ep", "tp", None),
        ),
        out_specs=P("ep", "tp"),
        check_vma=False,
    )
```

```python
import functools

import jax
import jax.numpy as jnp
import numpy as np
from jax import lax
from jax.experimental import pallas as pl
from jax.experimental.pallas import tpu as pltpu
from jax.sharding import PartitionSpec as P


BF = jnp.bfloat16
F32 = jnp.float32
SIDE = 4
TP = SIDE * SIDE
ROWS_BY_ROWS = (((1,), (1,)), ((), ()))
COLS_BY_COLS = (((0,), (0,)), ((), ()))


def flat_slots(routes, experts, capacity):
    tokens = routes.shape[1]
    first, second = routes[0:1, :], routes[1:2, :]
    expert = lax.broadcasted_iota(jnp.int32, (experts, tokens), 0)
    in_first, in_second = expert == first, expert == second
    named = jnp.where(in_first | in_second, 1.0, 0.0).astype(BF)
    earlier = lax.broadcasted_iota(jnp.int32, (tokens, tokens), 0)
    later = lax.broadcasted_iota(jnp.int32, (tokens, tokens), 1)
    before = jnp.dot(named, jnp.where(earlier < later, 1.0, 0.0).astype(BF), preferred_element_type=F32)
    place_first = jnp.sum(jnp.where(in_first, before, 0.0), axis=0, keepdims=True)
    place_second = jnp.sum(jnp.where(in_second, before, 0.0), axis=0, keepdims=True)
    return (
        first * capacity + place_first.astype(jnp.int32),
        second * capacity + place_second.astype(jnp.int32),
    )


def dispatch_body(routes, inputs, grads, out):
    experts, both, _ = out.shape
    capacity = both // 2
    tokens = inputs.shape[0]
    first, second = flat_slots(routes[...], experts, capacity)
    slot = lax.broadcasted_iota(jnp.int32, (experts * capacity, tokens), 0)
    pick = jnp.where((slot == first) | (slot == second), 1.0, 0.0).astype(BF)
    for at, source in ((0, inputs), (capacity, grads)):
        rows = jnp.dot(pick, source[...], preferred_element_type=F32).astype(BF)
        for e in range(experts):
            out[e, at : at + capacity] = rows[e * capacity : (e + 1) * capacity]


def combine_body(routes, shares, *refs):
    backs, out = refs[:-1], refs[-1]
    experts, part, _ = backs[0].shape
    capacity = part * len(backs)
    tokens = out.shape[0]
    first, second = flat_slots(routes[...], experts, capacity)
    slot = lax.broadcasted_iota(jnp.int32, (experts * capacity, tokens), 0)
    share = jnp.concatenate([shares[...], jnp.zeros((6, tokens), F32)], axis=0).T
    back = jnp.concatenate([ref[e] for e in range(experts) for ref in backs], axis=0)
    one = lax.dot_general(
        jnp.where(slot == first, 1.0, 0.0).astype(BF), back, COLS_BY_COLS, preferred_element_type=F32
    )
    two = lax.dot_general(
        jnp.where(slot == second, 1.0, 0.0).astype(BF), back, COLS_BY_COLS, preferred_element_type=F32
    )
    out[...] = (one * share[:, 0:1] + two * share[:, 1:2]).astype(out.dtype)


def weight_copies(x_order, g_order, hbm, vmem, here, first, count):
    (gate, up, down), (sides, downs), (sides_here, downs_here) = hbm, vmem, here
    width, units = gate.shape[1:]

    def for_acts(k):
        t = x_order[first * SIDE + k]
        return [
            pltpu.make_async_copy(gate.at[t], sides.at[k, :, :units], sides_here.at[0, k]),
            pltpu.make_async_copy(up.at[t], sides.at[k, :, units:], sides_here.at[1, k]),
        ]

    def for_hidden(i, f):
        t = g_order[(first + i) * SIDE + f]
        return pltpu.make_async_copy(
            down.at[:, pl.ds(pl.multiple_of(t * width, width), width)],
            downs.at[i, :, f * width : (f + 1) * width],
            downs_here.at[i, f],
        )

    def every():
        for i in range(count):
            for f in range(SIDE):
                yield from for_acts(i * SIDE + f)
            for f in range(SIDE):
                yield for_hidden(i, f)

    return for_acts, for_hidden, every


def absorb_body(x_order, g_order, *refs, first, count, ahead):
    pieces, refs = (refs[:2], refs[2:4]), refs[4:]
    given = first > 0
    before, refs = (refs[:4], refs[4:]) if given else ((), refs)
    hbm, outs, refs = refs[:3], refs[3:7], refs[7:]
    following = weight_copies(x_order, g_order, hbm, outs[2:], refs[:2], first + count, ahead)[2]
    if given:
        sides, downs = before[2:]
    else:
        sides, downs = refs[2:4]
        for_acts, for_hidden, every = weight_copies(x_order, g_order, hbm, refs[2:4], refs[4:6], first, count)
        for copy in every():
            copy.start()
    for copy in following():
        copy.start()
    wide = SIDE * hbm[0].shape[1]
    left = [jnp.concatenate([p[i] for p in pieces[kind] for i in range(p.shape[0])], axis=1) for kind in range(2)]
    if not given:
        for f in range(SIDE):
            for copy in for_acts(f):
                copy.wait()
    part = jnp.dot(left[0], sides[...].reshape(wide, sides.shape[2]), preferred_element_type=F32)
    outs[0][...] = before[0][...] + part if given else part
    if not given:
        for f in range(SIDE):
            for_hidden(0, f).wait()
    part = lax.dot_general(left[1], downs[0], ROWS_BY_ROWS, preferred_element_type=F32)
    outs[1][...] = before[1][...] + part if given else part
    for copy in following():
        copy.wait()


def finish_body(order, *refs):
    pieces, (acts, hidden, sides, downs, gate, up) = (refs[:2], refs[2:4]), refs[4:10]
    outs, later, (grads, wide, wide_here) = refs[10 : 10 + SIDE], refs[10 + SIDE], refs[11 + SIDE :]
    start_parts(order, gate, up, wide, wide_here)
    left = [jnp.concatenate([p[i] for p in pieces[kind] for i in range(p.shape[0])], axis=1) for kind in range(2)]
    right = sides[...].reshape(left[0].shape[1], sides.shape[2])
    form_grads(
        acts[...] + jnp.dot(left[0], right, preferred_element_type=F32),
        hidden[...] + lax.dot_general(left[1], downs[0], ROWS_BY_ROWS, preferred_element_type=F32),
        grads,
        later,
    )
    form_parts(order, grads, gate, up, wide, wide_here, outs)


def form_grads(acts, hidden, *outs):
    units = hidden.shape[1]
    gate, up = acts[:, :units], acts[:, units:]
    sigma = jax.nn.sigmoid(gate)
    slope = sigma * (1.0 + gate * (1.0 - sigma))
    for_gate = hidden * up * slope
    for_up = hidden * gate * sigma
    experts = outs[0].shape[0]
    start = 0
    for out in outs:
        part = out.shape[1]
        for b in range(experts):
            here = slice(b * hidden.shape[0] // experts + start, b * hidden.shape[0] // experts + start + part)
            out[b, :, :units] = for_gate[here].astype(BF)
            out[b, :, units:] = for_up[here].astype(BF)
        start += part


def part_copies(order, gate, up, sides, here, k):
    units = gate.shape[2]
    return [
        pltpu.make_async_copy(gate.at[order[k]], sides.at[k, :, :units], here.at[0, k]),
        pltpu.make_async_copy(up.at[order[k]], sides.at[k, :, units:], here.at[1, k]),
    ]


def start_parts(order, gate, up, sides, here):
    for k in range(TP):
        for copy in part_copies(order, gate, up, sides, here, k):
            copy.start()


def form_parts(order, grads, gate, up, sides, here, outs):
    experts, part_rows, both = grads.shape
    width = gate.shape[1]

    def members(j, carry):
        k = 2 * j
        for copy in part_copies(order, gate, up, sides, here, k) + part_copies(order, gate, up, sides, here, k + 1):
            copy.wait()
        part = lax.dot_general(
            grads[...].reshape(experts * part_rows, both),
            sides[pl.ds(k, 2)].reshape(2 * width, both),
            ROWS_BY_ROWS,
            preferred_element_type=F32,
        ).astype(BF)
        for f in range(SIDE):

            @pl.when(k // SIDE == f)
            def _():
                outs[f][k % SIDE] = part[:, :width]
                outs[f][k % SIDE + 1] = part[:, width:]

        return carry

    lax.fori_loop(0, TP // 2, members, 0)


def parts_body(order, grads, gate, up, *refs):
    outs, (sides, here) = refs[:SIDE], refs[SIDE:]
    start_parts(order, gate, up, sides, here)
    form_parts(order, grads, gate, up, sides, here, outs)


def vmem(mebibytes):
    return pltpu.CompilerParams(vmem_limit_bytes=mebibytes << 20)


def in_hbm(*arrays):
    return [pltpu.with_memory_space_constraint(a, pltpu.HBM) for a in arrays]


def z_shift(by):
    return [(z * SIDE + y, (z + by) % SIDE * SIDE + y) for z in range(SIDE) for y in range(SIDE)]


def y_shift(by):
    return [(z * SIDE + y, z * SIDE + (y + by) % SIDE) for z in range(SIDE) for y in range(SIDE)]


def shifted(x, shift, by):
    return lax.ppermute(x, "tp", shift(by))


def plane_gather(x, first, second):
    rows, width = x.shape
    below, above, far = [shifted(x, first, by) for by in (1, 3, 2)]
    halves = [jnp.concatenate([x, below], axis=0), jnp.concatenate([above, far], axis=0)]
    behind = [shifted(half, second, 1) for half in halves]
    ahead = [shifted(half, second, 3) for half in halves]
    away = [shifted(behind[0], second, 1), shifted(ahead[1], second, 3)]
    return [[half.reshape(2, rows, width) for half in ring] for ring in (halves, behind, ahead, away)]


def ring_sum(far, ahead, behind, own, shift):
    total = own.astype(F32)
    for by, part in ((2, far), (1, ahead), (3, behind)):
        total = total + shifted(part.astype(BF), shift, by).astype(F32)
    return total


def body(layer_input, out_grad, route, gate_share, gate_weight, up_weight, down_weight):
    experts = lax.axis_size("ep")
    tokens, width = layer_input.shape
    choose = route.shape[1]
    capacity = tokens * choose * 3 // (2 * experts)
    slots = experts * capacity
    parts = (7 * capacity // 12, 5 * capacity // 12)
    gate_matrix, up_matrix, down_matrix = gate_weight[0], up_weight[0], down_weight[0]
    _, units = gate_matrix.shape
    routes, shares = route.T, gate_share.T

    me = lax.axis_index("tp")
    z, y = me // SIDE, me % SIDE
    away = np.array([0, SIDE - 1, 1, 2], np.int32)
    ahead = np.array([2, 1, 3, 0], np.int32)

    def plane(outer, inner, z_outer):
        outer, inner = np.repeat(outer, SIDE), np.tile(inner, SIDE)
        in_z, in_y = (outer, inner) if z_outer else (inner, outer)
        return ((z + in_z) % SIDE * SIDE + (y + in_y) % SIDE).astype(jnp.int32)

    x_order, g_order = plane(away, away, False), plane(away, away, True)
    summed_order = [plane(ahead, np.arange(SIDE), True), plane(ahead, np.arange(SIDE), False)]

    sent = pl.pallas_call(
        dispatch_body,
        out_shape=jax.ShapeDtypeStruct((experts, 2 * capacity, width), BF),
        name="dispatch",
        compiler_params=vmem(16),
    )(routes, *in_hbm(layer_input, out_grad))
    got = lax.all_to_all(sent, "ep", split_axis=0, concat_axis=0, tiled=True)
    x = plane_gather(got[:, :capacity].reshape(slots, width), z_shift, y_shift)
    g = plane_gather(got[:, capacity:].reshape(slots, width), y_shift, z_shift)

    in_vmem = pl.BlockSpec(memory_space=pltpu.VMEM)
    in_smem = pl.BlockSpec(memory_space=pltpu.SMEM)
    stays = pl.BlockSpec(memory_space=pltpu.HBM)
    dma = pltpu.SemaphoreType.DMA
    sides_of = lambda count: pltpu.VMEM((count * SIDE, width, 2 * units), BF)
    downs_of = lambda count: pltpu.VMEM((count, units, SIDE * width), BF)
    blocks = in_hbm(gate_matrix.reshape(TP, width, units), up_matrix.reshape(TP, width, units), down_matrix)
    state = []
    for first, count, ahead, limit in ((0, 1, 1, 14), (1, 1, 1, 16), (2, 1, 1, 16)):
        used = [*x[first], *g[first], *state]
        own = []
        if first == 0:
            own = [sides_of(count), downs_of(count), dma((2, count * SIDE)), dma((count, SIDE))]
        state = pl.pallas_call(
            functools.partial(absorb_body, first=first, count=count, ahead=ahead),
            in_specs=[in_smem] * 2 + [in_vmem] * len(used) + [stays] * 3,
            out_specs=[in_vmem] * 4,
            out_shape=[
                jax.ShapeDtypeStruct((slots, 2 * units), F32),
                jax.ShapeDtypeStruct((slots, units), F32),
                jax.ShapeDtypeStruct((ahead * SIDE, width, 2 * units), BF),
                jax.ShapeDtypeStruct((ahead, units, SIDE * width), BF),
            ],
            scratch_shapes=[dma((2, ahead * SIDE)), dma((ahead, SIDE))] + own,
            name="absorb",
            compiler_params=vmem(limit),
        )(x_order, g_order, *used, *blocks)

    def parts_shape(part):
        return [jax.ShapeDtypeStruct((SIDE, experts * part, width), BF)] * SIDE

    summed = []
    for h, part in enumerate(parts):
        if h == 0:
            later_shape = jax.ShapeDtypeStruct((experts, parts[1], 2 * units), BF)
            *outs, later = pl.pallas_call(
                finish_body,
                in_specs=[in_smem] + [in_vmem] * 8 + [stays] * 2,
                out_specs=[in_vmem] * (SIDE + 1),
                out_shape=parts_shape(part) + [later_shape],
                scratch_shapes=[pltpu.VMEM((experts, part, 2 * units), BF), sides_of(SIDE), dma((2, TP))],
                name="finish",
                compiler_params=vmem(29),
            )(summed_order[h], *x[3], *g[3], *state, *blocks[:2])
        else:
            outs = pl.pallas_call(
                parts_body,
                in_specs=[in_smem, in_vmem] + [stays] * 2,
                out_specs=[in_vmem] * SIDE,
                out_shape=parts_shape(part),
                scratch_shapes=[sides_of(SIDE), dma((2, TP))],
                name="parts",
                compiler_params=vmem(28),
            )(summed_order[h], later, *blocks[:2])
        first, second = (z_shift, y_shift) if h == 0 else (y_shift, z_shift)
        line = ring_sum(*outs, first)
        mine = ring_sum(line[2], line[1], line[3], line[0], second)
        summed.append(mine.astype(BF).reshape(experts, part, width))
    backs = [
        lax.all_to_all(jnp.concatenate(summed, axis=1), "ep", split_axis=0, concat_axis=0, tiled=True)
    ]

    return pl.pallas_call(
        combine_body,
        out_shape=jax.ShapeDtypeStruct((tokens, width), BF),
        name="combine",
        compiler_params=vmem(16),
    )(routes, shares, *backs)


def solution(mesh):
    return jax.shard_map(
        body,
        mesh=mesh,
        in_specs=(
            P("ep", "tp"),
            P("ep", "tp"),
            P("ep", None),
            P("ep", None),
            P("ep", None, "tp"),
            P("ep", None, "tp"),
            P("ep", "tp", None),
        ),
        out_specs=P("ep", "tp"),
        check_vma=False,
    )
```
